32 devices in a mesh: seq: 16 (over z, x, core), head: 2 (over y).
Axes of the slice: x: 2, y: 2, z: 4, core: 2. Of those that a mesh axis runs over, the one named last changes fastest.
Arguments:
- x_proj: bfloat16 [4096, 8192], P(('seq', 'head')), may hold values from -6 to 6
- z_proj: bfloat16 [4096, 8192], P(('seq', 'head')), may hold values from -6 to 6
- b_proj: bfloat16 [4096, 1024], P(('seq', 'head')), may hold values from -6 to 6
- c_proj: bfloat16 [4096, 1024], P(('seq', 'head')), may hold values from -6 to 6
- dt_raw: bfloat16 [4096, 128], P(('seq', 'head')), may hold values from -3.2 to 3.2, as said below
- dt_bias: float32 [128], P('head'), may hold values from -6.3 to -1.2, as said below
- a_log: float32 [128], P('head'), as said below
- d_skip: float32 [128], P('head'), may hold values from 0.5 to 2
- conv_x: float32 [4, 8192], P(None, 'head'), may hold values from -3 to 3
- conv_bias_x: float32 [8192], P('head'), may hold values from -3 to 3
- conv_bc: float32 [4, 2, 1024], P(None, None, 'head'), may hold values from -3 to 3
- conv_bias_bc: float32 [2, 1024], P(None, 'head'), may hold values from -3 to 3
- norm_weight: float32 [8192], P('head'), may hold values from 0.25 to 1.75
- out_weight: bfloat16 [8192, 4096], P('head', 'seq'), may hold values from -0.0625 to 0.0625
Outputs:
- mixed: bfloat16 [4096, 4096], P(('seq', 'head'))
The draws below stay inside these ranges and needn't reach their ends.
Inputs may be any that keep to these rules, and one draw needn't show every extreme that they name: `dt_raw`: A normal draw times 0.7 plus an offset common to each head and each aligned run of 256 tokens. `dt_bias`: the inverse softplus of a per-head step size between 0.002 and 0.25. Finite; exp(a_log) lies above 0.0 and at most 0.3.
All inputs are finite; a program needn't handle non-finite values.
Results may differ from the reference program's by a relative error of at most 0.014.
Values may be sent and summed in bfloat16 or wider, within the bound.
A program may use at most 192 MiB of HBM per device.

```python
import jax
import jax.numpy as jnp
from jax import lax

D = 4096
HEADS = 128
HEAD_DIM = 64
STATE = 128
GROUPS = 8
CONV = 4
TOK_DEV = 256
SPAN = 128
DI = 8192
TOKENS = 4096
N_HEAD = 2


def head_kinds(key):
    order = jax.random.permutation(jax.random.fold_in(key, 101), HEADS)
    return order < HEADS // 2


def draw_dt_bias(key, part):
    slow_heads = head_kinds(key)
    uniform_draw = jax.random.uniform(jax.random.fold_in(key, 102), (HEADS,), jnp.float32)
    lower_log = jnp.where(slow_heads, jnp.log(0.002), jnp.log(0.08))
    upper_log = jnp.where(slow_heads, jnp.log(0.006), jnp.log(0.25))
    step_value = jnp.exp(lower_log + uniform_draw * (upper_log - lower_log))
    return jnp.log(jnp.expm1(step_value)).astype(jnp.float32)


def draw_a_log(key, part):
    slow_heads = head_kinds(key)
    uniform_draw = jax.random.uniform(jax.random.fold_in(key, 105), (HEADS,), jnp.float32)
    slow_log = jnp.log(0.1) + uniform_draw * (jnp.log(0.6) - jnp.log(0.1)) - jnp.log(0.004 * TOKENS)
    fast_log = jnp.log(0.15) + uniform_draw * (jnp.log(0.3) - jnp.log(0.15))
    return jnp.where(slow_heads, slow_log, fast_log).astype(jnp.float32)


def draw_dt_raw(key, part):
    noise_part = jax.random.truncated_normal(jax.random.fold_in(key, 103), -3.0, 3.0, (TOKENS, HEADS), jnp.float32) * 0.7
    offsets = jax.random.uniform(jax.random.fold_in(key, 104), (TOKENS // TOK_DEV, HEADS), jnp.float32, minval=-1.0, maxval=1.0)
    return (noise_part + jnp.repeat(offsets, TOK_DEV, axis=0)).astype(jnp.bfloat16)


def block_levels(own_key, shape, pieces, smallest, high):
    loudness = 1.0
    for axis_at, shards_of in pieces:
        steps = jax.random.uniform(jax.random.fold_in(jax.random.fold_in(own_key, 6), axis_at), (shards_of,), jnp.float32, smallest / len(pieces), high / len(pieces))
        loudness = loudness * jnp.repeat(jnp.exp(steps), shape[axis_at] // shards_of).reshape((-1,) + (1,) * (len(shape) - 1 - axis_at))
    return loudness


def normal_values(stream_key, extent, scale, most, split=(), held_as=jnp.bfloat16):
    gain = block_levels(stream_key, extent, split, -0.22, 0.18) if split else 1.0
    array = jax.random.normal(stream_key, extent, jnp.float32) * scale * gain
    return jnp.minimum(jnp.maximum(array, -most), most).astype(held_as)


def setup_inputs(seed: int = 0) -> dict:
    key_of = jax.random.split(jax.random.key(seed), 15)
    x_proj = normal_values(key_of[0], (TOKENS, DI), 1.0, 6.0, ((0, 32),))
    z_proj = normal_values(key_of[1], (TOKENS, DI), 1.0, 6.0, ((0, 32),))
    b_proj = normal_values(key_of[2], (TOKENS, GROUPS * STATE), 1.0, 6.0, ((0, 32),))
    c_proj = normal_values(key_of[3], (TOKENS, GROUPS * STATE), 1.0, 6.0, ((0, 32),))
    dt_raw = draw_dt_raw(jax.random.fold_in(key_of[14], 71), 0)
    dt_bias = draw_dt_bias(jax.random.fold_in(key_of[14], 71), 0)
    a_log = draw_a_log(jax.random.fold_in(key_of[14], 71), 0)
    d_skip = jnp.clip(0.5 + 1.5 * jax.random.uniform(key_of[7], (HEADS,), jnp.float32) ** block_levels(key_of[7], (HEADS,), ((0, 2),), -0.2, 0.2), 0.5, 2.0)
    conv_x = normal_values(key_of[8], (CONV, DI), CONV ** -0.5, 3.0, ((1, 2),), jnp.float32)
    conv_bias_x = normal_values(key_of[9], (DI,), 0.5, 3.0, ((0, 2),), jnp.float32)
    conv_bc = normal_values(key_of[10], (CONV, 2, GROUPS * STATE), CONV ** -0.5, 3.0, ((2, 2),), jnp.float32)
    conv_bias_bc = normal_values(key_of[11], (2, GROUPS * STATE), 0.5, 3.0, ((1, 2),), jnp.float32)
    norm_weight = jnp.clip(1.0 + 0.15 * jax.random.normal(key_of[12], (DI,), jnp.float32), 0.25, 1.75)
    out_weight = normal_values(key_of[13], (DI, D), DI ** -0.5, 0.0625, ((0, 2), (1, 16)))
    return {"x_proj": x_proj, "z_proj": z_proj, "b_proj": b_proj, "c_proj": c_proj, "dt_raw": dt_raw, "dt_bias": dt_bias, "a_log": a_log, "d_skip": d_skip, "conv_x": conv_x, "conv_bias_x": conv_bias_x, "conv_bc": conv_bc, "conv_bias_bc": conv_bias_bc, "norm_weight": norm_weight, "out_weight": out_weight}


def conv_silu(inputs, weight, bias_row):
    taps = weight.shape[0]
    padded = jnp.pad(inputs.astype(jnp.float32), ((taps - 1, 0), (0, 0)))
    length = inputs.shape[0]
    summed = jnp.broadcast_to(bias_row, inputs.shape).astype(jnp.float32)
    for offset in range(taps):
        summed = summed + weight[offset] * padded[offset:offset + length]
    return jax.nn.silu(summed).astype(jnp.bfloat16)

def to_bf16_f32(value):
    rounded = lax.optimization_barrier(value.astype(jnp.bfloat16))
    return rounded.astype(jnp.float32)

def reference(x_proj, z_proj, b_proj, c_proj, dt_raw, dt_bias, a_log, d_skip, conv_x, conv_bias_x, conv_bc, conv_bias_bc, norm_weight, out_weight):
    high = lax.Precision.HIGHEST
    x_conv = conv_silu(x_proj, conv_x, conv_bias_x)
    b_conv = conv_silu(b_proj, conv_bc[:, 0], conv_bias_bc[0])
    c_conv = conv_silu(c_proj, conv_bc[:, 1], conv_bias_bc[1])
    step_size = jax.nn.softplus(dt_raw.astype(jnp.float32) + dt_bias)
    coeff = -jnp.exp(a_log)
    blocks = TOKENS // SPAN
    per_group = HEADS // GROUPS
    x_blocks = x_conv.reshape(blocks, SPAN, HEADS, HEAD_DIM)
    b_blocks = b_conv.reshape(blocks, SPAN, GROUPS, STATE)
    c_blocks = c_conv.reshape(blocks, SPAN, GROUPS, STATE)
    step_blocks = step_size.reshape(blocks, SPAN, HEADS)
    causal = jnp.arange(SPAN)[:, None] >= jnp.arange(SPAN)[None, :]

    def span_step(state, inputs):
        x_span, b_span, c_span, step_span = inputs
        x_float = x_span.astype(jnp.float32)
        b_float = b_span.astype(jnp.float32)
        c_float = c_span.astype(jnp.float32)
        cumulative = jnp.cumsum(coeff * step_span, axis=0)
        scores = jnp.einsum('tgn,sgn->gts', c_float, b_float, precision=high)
        by_head = cumulative.T
        spread = by_head[:, :, None] - by_head[:, None, :]
        decays = jnp.exp(jnp.where(causal, spread, -jnp.inf))
        scaled = decays * step_span.T[:, None, :]
        mix_weights = (scaled.reshape(GROUPS, per_group, SPAN, SPAN) * scores[:, None]).reshape(HEADS, SPAN, SPAN)
        mix_weights = to_bf16_f32(mix_weights)
        y_local = jnp.einsum('hts,shp->thp', mix_weights, x_float, precision=high)
        state_scale = step_span * jnp.exp(cumulative[-1:] - cumulative)
        x_weighted = to_bf16_f32(x_float * state_scale[:, :, None])
        piece = jnp.einsum('sgqp,sgn->gqpn', x_weighted.reshape(SPAN, GROUPS, per_group, HEAD_DIM), b_float, precision=high)
        piece = piece.reshape(HEADS, HEAD_DIM, STATE)
        start_state = to_bf16_f32(state).reshape(GROUPS, per_group, HEAD_DIM, STATE)
        y_carry = jnp.einsum('tgn,gqpn->tgqp', c_float, start_state, precision=high).reshape(SPAN, HEADS, HEAD_DIM)
        y_carry = y_carry * jnp.exp(cumulative)[:, :, None]
        outputs = y_local + y_carry + d_skip[:, None] * x_float
        new_state = jnp.exp(cumulative[-1])[:, None, None] * state + piece
        return (new_state, outputs)
    initial = jnp.zeros((HEADS, HEAD_DIM, STATE), jnp.float32)
    final_state, outputs = lax.scan(span_step, initial, (x_blocks, b_blocks, c_blocks, step_blocks))
    outputs = outputs.reshape(TOKENS, DI)
    gated = outputs * jax.nn.silu(z_proj.astype(jnp.float32))
    grouped = gated.reshape(TOKENS, GROUPS, DI // GROUPS)
    normed = grouped / jnp.sqrt(lax.optimization_barrier(jnp.mean(grouped * grouped, axis=-1, keepdims=True)) + 1.0)
    normed = (normed.reshape(TOKENS, DI) * norm_weight).astype(jnp.bfloat16)
    block_rows = DI // N_HEAD
    summed = jnp.zeros((TOKENS, D), jnp.float32)
    for block_idx in range(N_HEAD):
        rows_lo = block_idx * block_rows
        partial_sum = jnp.dot(normed[:, rows_lo:rows_lo + block_rows], out_weight[rows_lo:rows_lo + block_rows], preferred_element_type=jnp.float32)
        summed = summed + to_bf16_f32(partial_sum)
    return summed.astype(jnp.bfloat16)
```

```python
import functools
import types

import jax
import jax.numpy as jnp
from jax import lax
from jax.experimental import pallas as pl
from jax.experimental.pallas import tpu as pltpu
from jax.sharding import PartitionSpec as P

HEAD_DIM = 64
STATE = 128
SPAN = 128
HALO = 16
INNER = 4
CHUNKS = 16
STEPS = 8
AHEAD = 3
LANES = 128
NT = (((1,), (1,)), ((), ()))
MESH = pl.DeviceIdType.MESH


def relay_passes(outer):
    passes = 0
    for level in range(outer):
        room = outer - 1 - level
        behind = level // 2 + 1
        if room >= 1:
            passes = max(passes, behind * min(room, 2))
    return passes


def column_order(outer):
    evens = list(range(0, outer, 2))
    odds = list(range(1, outer, 2))
    return evens + odds


def conv_silu(value, halo, taps_of, bias, padded, dtype):
    tokens = value.shape[0]
    padded[0:8, :] = halo.astype(jnp.float32)
    padded[8 : 8 + tokens, :] = value.astype(jnp.float32)
    total = bias + jnp.zeros(value.shape, jnp.float32)
    taps = len(taps_of)
    for offset in range(taps):
        low = 8 - (taps - 1) + offset
        total = total + taps_of[offset] * padded[low : low + tokens, :]
    return (total / (1.0 + jnp.exp(-total))).astype(dtype)


def mixer_kernel(count, heads, names, *refs):
    r = types.SimpleNamespace(**dict(zip(names, refs)))
    seq = lax.axis_index("seq")
    head = lax.axis_index("head")
    outer = count // INNER
    inner = lax.rem(seq, INNER)
    level = lax.div(seq, INNER)
    rows = r.x_in.shape[0]
    tokens = rows * heads
    groups, _, width = r.x_buf.shape
    per = width // HEAD_DIM
    blocks = tokens // SPAN
    local_heads = groups * per
    part = width // INNER
    part_heads = part // HEAD_DIM
    depth = r.wv.shape[1]
    tile = r.wv.shape[2]
    chunk_rows = depth // CHUNKS
    step_rows = depth // STEPS
    passes = relay_passes(outer)
    taps = r.conv_x.shape[0]
    dtype = r.x_buf.dtype

    near = seq + 1 - 2 * lax.rem(seq, 2)
    side = seq + 2 - 4 * lax.rem(lax.div(seq, 2), 2)
    cross = near + side - seq
    mates = (seq, near, side, cross)
    inners = tuple(lax.rem(mate, INNER) for mate in mates)

    def remote(source, target, send, recv, device):
        return pltpu.make_async_remote_copy(
            src_ref=source,
            dst_ref=target,
            send_sem=send,
            recv_sem=recv,
            device_id=device,
            device_id_type=MESH,
        )

    def head_of(step):
        return lax.rem(head + step, heads)

    barrier = pltpu.get_barrier_semaphore()
    gives_halo = jnp.logical_and(head == heads - 1, seq < count - 1)
    takes_halo = seq > 0
    gives_out = jnp.logical_and(gives_halo, inner == INNER - 1)
    takes_out = jnp.logical_and(takes_halo, inner == 0)

    def greet(where, which):
        pl.semaphore_signal(barrier, inc=1, device_id=(where, which), device_id_type=MESH)

    for index, mate in enumerate(mates):
        for step in range(heads):
            if index or step:
                greet(mate, head_of(step))
    expected = jnp.int32(INNER * heads - 1)
    for sign in (1, -1):
        for distance in (1, 2):
            there = level + sign * distance
            exists = jnp.logical_and(there >= 0, there < outer)

            @pl.when(exists)
            def _(there=there):
                greet(there * INNER + inner, head)

            expected = expected + jnp.where(exists, 1, 0)

    @pl.when(gives_out)
    def _():
        for which in range(heads):
            greet(seq + 1, which)

    @pl.when(takes_out)
    def _():
        greet(seq - 1, heads - 1)

    expected = expected + jnp.where(gives_out, heads, 0) + jnp.where(takes_out, 1, 0)
    pl.semaphore_wait(barrier, expected)

    mine = pl.ds(pl.multiple_of(head * rows, 16), rows)
    plan = (
        (r.b_in, r.b_buf, STATE),
        (r.c_in, r.c_buf, STATE),
        (r.x_in, r.x_buf, width),
        (r.z_in, r.z_buf, width),
    )
    halos = ((r.x_in, r.x_halo), (r.b_in, r.b_halo), (r.c_in, r.c_halo))

    def halo_copy(index, which, device):
        source, target = halos[index]
        size = target.shape[1]
        return remote(
            source.at[pl.ds(rows - HALO, HALO), pl.ds(which * size, size)],
            target,
            r.halo_send.at[index, which],
            r.halo_recv.at[index],
            device,
        )

    def entry_view(kind, which, g):
        source, target, size = plan[kind]
        low = pl.multiple_of((which * groups + g) * size, LANES)
        return source.at[:, pl.ds(low, size)], target.at[g, mine]

    def entry_copy(kind, g, step):
        source, target = entry_view(kind, head_of(step), g)
        return remote(
            source,
            target,
            r.entry_send.at[kind, step, g],
            r.entry_recv.at[kind, step, g],
            (seq, head_of(step)),
        )

    def own_copy(kind, g):
        source, target = entry_view(kind, head, g)
        return pltpu.make_async_copy(source, target, r.own_sems.at[kind, g])

    def dt_copy(step):
        return remote(
            r.dt_in,
            r.dt_buf.at[mine],
            r.dt_send.at[step],
            r.dt_recv.at[step],
            (seq, head_of(step)),
        )

    own_dt = pltpu.make_async_copy(r.dt_in, r.dt_buf.at[mine], r.misc_sems.at[0])
    own_weight = pltpu.make_async_copy(r.w_in, r.wv.at[level], r.misc_sems.at[1])

    own_dt.start()
    for step in range(1, heads):
        dt_copy(step).start()
    own_weight.start()

    @pl.when(gives_halo)
    def _():
        for index in range(len(halos)):
            for which in range(heads):
                halo_copy(index, which, (seq + 1, which)).start()

    for g in range(groups):
        for kind in range(3):
            own_copy(kind, g).start()
            for step in range(1, heads):
                entry_copy(kind, g, step).start()
    for g in range(groups):
        own_copy(3, g).start()
        for step in range(1, heads):
            entry_copy(3, g, step).start()

    def weight_item(sign, which, chunk, act):
        room = outer - 1 - level if sign > 0 else level
        behind = lax.div(level if sign > 0 else outer - 1 - level, 2)
        far = room >= 2
        hops = jnp.where(far, lax.div(which, 2), which)
        distance = jnp.where(far, 2 - lax.rem(which, 2), 1)
        exists = jnp.logical_and(room >= 1, hops <= behind)
        block = level - sign * 2 * hops
        target = (level + sign * distance) * INNER + inner
        view = r.wv.at[block, pl.ds(pl.multiple_of(chunk * chunk_rows, 16), chunk_rows)]
        copy = remote(
            view,
            view,
            r.weight_send.at[0 if sign > 0 else 1, which, chunk],
            r.weight_recv.at[block, chunk],
            (target, head),
        )
        if act == "wait":

            @pl.when(exists)
            def _():
                copy.wait_send()

            return
        fresh = jnp.logical_or(jnp.logical_not(far), distance == 2)
        relayed = jnp.logical_and(jnp.logical_and(exists, hops >= 1), fresh)

        @pl.when(relayed)
        def _():
            copy.wait_recv()

        @pl.when(exists)
        def _():
            copy.start()

    def weight_pass(which, chunk):
        if passes:
            weight_item(1, which, chunk, "start")
            weight_item(-1, which, chunk, "start")

    def weight_arrived(block, chunk):
        below = block < level
        apart = jnp.where(below, level - block, block - level)
        room = jnp.where(below, outer - 1 - level, level)
        relayed = jnp.logical_and(lax.rem(apart, 2) == 0, room >= 1)

        @pl.when(jnp.logical_and(apart > 0, jnp.logical_not(relayed)))
        def _():
            view = r.wv.at[block, pl.ds(pl.multiple_of(chunk * chunk_rows, 16), chunk_rows)]
            remote(
                view,
                view,
                r.weight_send.at[0, 0, chunk],
                r.weight_recv.at[block, chunk],
                (seq, head),
            ).wait_recv()

    own_weight.wait()
    for chunk in range(AHEAD):
        weight_pass(0, chunk)

    r.params[...] = jnp.zeros_like(r.params)
    r.params[0:1, 0:local_heads] = r.dt_bias[...]
    r.params[1:2, 0:local_heads] = r.a_log[...]
    columns = r.params[...].T
    bias = columns[0:local_heads, 0:1]
    coeff = -jnp.exp(columns[0:local_heads, 1:2])
    own_dt.wait()
    for step in range(1, heads):
        dt_copy(step).wait_recv()
    early = lax.broadcasted_iota(jnp.int32, (SPAN, SPAN), 0)
    late = lax.broadcasted_iota(jnp.int32, (SPAN, SPAN), 1)
    prefix_ones = jnp.where(early <= late, 1.0, 0.0).astype(jnp.float32)
    r.cum_pad[...] = jnp.zeros_like(r.cum_pad)
    log_total = jnp.zeros((1, LANES), jnp.float32)
    for block in range(blocks):
        span = slice(block * SPAN, (block + 1) * SPAN)
        r.dt_t[...] = r.dt_buf[span, :].astype(jnp.float32).T
        raw = r.dt_t[pl.ds(pl.multiple_of(head * local_heads, 8), local_heads), :] + bias
        step_size = jnp.maximum(raw, 0.0) + jnp.log1p(jnp.exp(-jnp.abs(raw)))
        r.step_t[:, span] = step_size
        summed = jnp.dot(
            coeff * step_size,
            prefix_ones,
            preferred_element_type=jnp.float32,
            precision=lax.Precision.HIGHEST,
        )
        r.cum_t[:, span] = summed
        r.cum_pad[0:local_heads, :] = summed
        by_token = r.cum_pad[...].T
        log_total = log_total + by_token[SPAN - 1 : SPAN, :]
        for g in range(groups):
            shift = (LANES - g * per) % LANES
            r.cum_c[g, span, :] = pltpu.roll(by_token, shift, 1) if shift else by_token
    logs = jnp.broadcast_to(log_total, (8, LANES))
    r.log_out[...] = logs
    r.log_in[inner] = logs

    def log_copy(index):
        return remote(
            r.log_out,
            r.log_in.at[inner],
            r.log_send.at[index],
            r.log_recv.at[index],
            (mates[index], head),
        )

    for index in range(1, INNER):
        log_copy(index).start()

    @pl.when(jnp.logical_not(takes_halo))
    def _():
        for _, target in halos:
            target[...] = jnp.zeros_like(target)

    @pl.when(takes_halo)
    def _():
        for index in range(len(halos)):
            halo_copy(index, 0, (seq, head)).wait_recv()

    @pl.when(level == 0)
    def _():
        r.chain_in[...] = jnp.zeros_like(r.chain_in)

    causal = early >= late

    def piece_copy(g, index):
        low = pl.multiple_of(inners[index] * part, 16)
        return remote(
            r.final_out.at[g, pl.ds(low, part)],
            r.piece_in.at[g, inner],
            r.piece_send.at[g, index],
            r.piece_recv.at[g, index],
            (mates[index], head),
        )

    def local(g, carry):
        for kind in range(3):
            own_copy(kind, g).wait()
            for step in range(1, heads):
                entry_copy(kind, g, step).wait_recv()
        wide = pl.ds(pl.multiple_of(g * width, LANES), width)
        slim = pl.ds(pl.multiple_of(g * STATE, LANES), STATE)
        x_conv = conv_silu(
            r.x_buf[g],
            r.x_halo[HALO - 8 : HALO, wide],
            [r.conv_x[tap : tap + 1, wide] for tap in range(taps)],
            r.bias_x[:, wide],
            r.x_pad,
            dtype,
        )
        b_conv = conv_silu(
            r.b_buf[g],
            r.b_halo[HALO - 8 : HALO, slim],
            [r.conv_bc[tap, 0:1, slim] for tap in range(taps)],
            r.bias_bc[0:1, slim],
            r.bc_pad,
            dtype,
        )
        c_conv = conv_silu(
            r.c_buf[g],
            r.c_halo[HALO - 8 : HALO, slim],
            [r.conv_bc[tap, 1:2, slim] for tap in range(taps)],
            r.bias_bc[1:2, slim],
            r.bc_pad,
            dtype,
        )
        r.c_conv[g] = c_conv
        own_heads = pl.ds(pl.multiple_of(g * per, 8), per)
        for block in range(blocks):
            low = block * SPAN
            b_blk = b_conv[low : low + SPAN]
            c_blk = c_conv[low : low + SPAN]
            r.x_t[...] = x_conv[low : low + SPAN].astype(jnp.float32).T
            scores = lax.dot_general(c_blk, b_blk, NT, preferred_element_type=jnp.float32)
            cum_rows = r.cum_t[own_heads, low : low + SPAN]
            step_all = r.step_t[own_heads, low : low + SPAN]
            for index in range(per):
                lines = pl.ds(index * HEAD_DIM, HEAD_DIM)
                column = r.cum_c[g, low : low + SPAN, index : index + 1]
                row = cum_rows[index : index + 1, :]
                step = step_all[index : index + 1, :]
                total = row[:, SPAN - 1 : SPAN]
                decays = jnp.exp(jnp.where(causal, column - row, -jnp.inf))
                mix = (decays * step * scores).astype(dtype)
                x_head = r.x_t[lines, :]
                product = lax.dot_general(
                    x_head.astype(dtype), mix, NT, preferred_element_type=jnp.float32
                )
                r.y_t[g, block, lines, :] = product + r.skip[g * per + index] * x_head
                r.x_w[lines, :] = (x_head * (step * jnp.exp(total - row))).astype(dtype)
            piece = jnp.dot(r.x_w[...], b_blk, preferred_element_type=jnp.float32)
            if block < blocks - 1:
                r.pieces[g, block] = piece
            if block == 0:
                r.final[...] = piece
            else:
                r.running[...] = piece
                for index in range(per):
                    lines = pl.ds(index * HEAD_DIM, HEAD_DIM)
                    decay = jnp.exp(cum_rows[index : index + 1, SPAN - 1 : SPAN])
                    r.final[lines, :] = decay * r.final[lines, :] + r.running[lines, :]
        r.final_out[g] = r.final[...].astype(dtype)
        for index in range(1, INNER):
            piece_copy(g, index).start()
        own_part = pl.ds(pl.multiple_of(inner * part, 16), part)
        r.piece_in[g, inner] = r.final_out[g, own_part, :]
        weight_pass(0, AHEAD + g)
        return carry

    lax.fori_loop(0, groups, local, 0)

    def chain_copy(g, where):
        return remote(
            r.chain_out.at[g],
            r.chain_in.at[g],
            r.chain_send.at[g],
            r.chain_recv.at[g],
            (where, head),
        )

    def start_copy(g, index):
        low = pl.multiple_of(inner * part, 16)
        return remote(
            r.start_out.at[g, inners[index]],
            r.start_in.at[g, pl.ds(low, part)],
            r.start_send.at[g, index],
            r.start_recv.at[g, index],
            (mates[index], head),
        )

    for index in range(1, INNER):
        log_copy(index).wait_recv()

    def carry_step(g, carry):
        for index in range(1, INNER):
            piece_copy(g, index).wait_recv()

        @pl.when(level > 0)
        def _():
            chain_copy(g, seq).wait_recv()

        first = g * per + inner * part_heads
        state = [
            r.chain_in[g, index * HEAD_DIM : (index + 1) * HEAD_DIM, :].astype(jnp.float32)
            for index in range(part_heads)
        ]
        for position in range(INNER):
            decays = jnp.exp(pltpu.roll(r.log_in[position], lax.rem(LANES - first, LANES), 1))
            for index in range(part_heads):
                lines = slice(index * HEAD_DIM, (index + 1) * HEAD_DIM)
                r.start_out[g, position, lines, :] = state[index].astype(dtype)
                piece = r.piece_in[g, position, lines, :].astype(jnp.float32)
                state[index] = decays[0:1, index : index + 1] * state[index] + piece
        for index in range(part_heads):
            r.chain_out[g, index * HEAD_DIM : (index + 1) * HEAD_DIM, :] = state[index].astype(
                dtype
            )

        @pl.when(level < outer - 1)
        def _():
            chain_copy(g, seq + INNER).start()

        for index in range(1, INNER):
            start_copy(g, index).start()
        own_part = pl.ds(pl.multiple_of(inner * part, 16), part)
        r.start_in[g, own_part, :] = r.start_out[g, inner]
        weight_pass(0, AHEAD + groups + g)
        return carry

    lax.fori_loop(0, groups, carry_step, 0)

    def share_copy(g, index):
        target = r.a_buf.at[g, pl.ds(index * tokens, tokens)]
        return remote(
            r.a_buf.at[g, pl.ds(0, tokens)],
            target,
            r.share_send.at[g, index],
            r.share_recv.at[g, index],
            (mates[index], head),
        )

    def forward_copy(g):
        return remote(
            r.a_buf.at[g, pl.ds(2 * tokens, tokens)],
            r.a_buf.at[g, pl.ds(3 * tokens, tokens)],
            r.share_send.at[g, 3],
            r.share_recv.at[g, 3],
            (near, head),
        )

    def norm_step(g, carry):
        for index in range(1, INNER):
            start_copy(g, index).wait_recv()
        own_copy(3, g).wait()
        for step in range(1, heads):
            entry_copy(3, g, step).wait_recv()
        wide = pl.ds(pl.multiple_of(g * width, LANES), width)
        own_heads = pl.ds(pl.multiple_of(g * per, 8), per)
        r.running[...] = r.start_in[g].astype(jnp.float32)
        for block in range(blocks):
            low = block * SPAN
            c_blk = r.c_conv[g, low : low + SPAN, :]
            r.x_t[...] = lax.dot_general(
                r.running[...].astype(dtype), c_blk, NT, preferred_element_type=jnp.float32
            )
            grown = jnp.exp(r.cum_t[own_heads, low : low + SPAN])
            for index in range(per):
                lines = pl.ds(index * HEAD_DIM, HEAD_DIM)
                row = grown[index : index + 1, :]
                r.x_t[lines, :] = r.y_t[g, block, lines, :] + r.x_t[lines, :] * row
                if block < blocks - 1:
                    r.running[lines, :] = (
                        row[:, SPAN - 1 : SPAN] * r.running[lines, :]
                        + r.pieces[g, block, lines, :]
                    )
            gate = r.z_buf[g, low : low + SPAN, :].astype(jnp.float32)
            gated = r.x_t[...].T * (gate / (1.0 + jnp.exp(-gate)))
            mean = jnp.sum(gated * gated, axis=-1, keepdims=True) * (1.0 / width)
            normed = gated * lax.rsqrt(mean + 1.0)
            r.a_buf[g, low : low + SPAN, :] = (normed * r.gain[:, wide]).astype(dtype)
        share_copy(g, 2).start()
        share_copy(g, 1).start()
        weight_pass(0, AHEAD + 2 * groups + g)
        return carry

    lax.fori_loop(0, groups, norm_step, 0)

    def rest(which, low):
        def body(chunk, carry):
            weight_pass(which, chunk)
            return carry

        lax.fori_loop(low, CHUNKS, body, 0)

    rest(0, min(AHEAD + 3 * groups, CHUNKS))

    def later_pass(which, carry):
        rest(which, 0)
        return carry

    if passes > 1:
        lax.fori_loop(1, passes, later_pass, 0)

    order = column_order(outer)
    early_count = (outer + 1) // 2
    direction = jnp.where(level < (outer + 1) // 2, 1, -1)

    def block_at(index):
        return lax.rem(level + direction * order[index] + outer, outer)

    steps_per_group = width // step_rows

    def product(block, step, low, size):
        g = lax.div(step, steps_per_group)
        off = pl.multiple_of(lax.rem(step, steps_per_group) * step_rows, LANES)
        down = pl.multiple_of(step * step_rows, 16)
        return jnp.dot(
            r.a_buf[g, low : low + size, pl.ds(off, step_rows)],
            r.wv[block, pl.ds(down, step_rows), :],
            preferred_element_type=jnp.float32,
        )

    per_step = CHUNKS // STEPS

    def arrive(block, step):
        for extra in range(per_step):
            weight_arrived(block, step * per_step + extra)

    def result_copy(index, mate, which):
        low = pl.multiple_of(mate * tokens + which * rows, 16)
        return remote(
            r.terms.at[index, pl.ds(low, rows)],
            r.landed.at[head, block_at(index) * INNER + inner],
            r.term_send.at[index, mate, which],
            r.term_recv.at[head, block_at(index) * INNER + inner],
            (mates[mate], which),
        )

    def ship(index, low_mate, mate_count):
        for mate in range(low_mate, low_mate + mate_count):
            for which in range(heads):
                if mate == 0:

                    @pl.when(head != which)
                    def _(mate=mate, which=which):
                        result_copy(index, mate, which).start()

                else:
                    result_copy(index, mate, which).start()
        if low_mate == 0:
            own_rows = pl.ds(pl.multiple_of(head * rows, 16), rows)
            r.landed[head, block_at(index) * INNER + inner] = r.terms[index, own_rows, :]

    half = 2 * tokens

    def unit(index, low, waits):
        block = block_at(index)
        r.acc[0, 0:half, :] = jnp.zeros((half, tile), jnp.float32)

        def body(step, carry):
            if waits:
                arrive(block, step)
            r.acc[0, 0:half, :] += product(block, step, low, half)
            return carry

        lax.fori_loop(0, STEPS, body, 0)
        r.terms[index, low : low + half, :] = r.acc[0, 0:half, :].astype(dtype)

    for g in range(groups):
        share_copy(g, 1).wait_recv()
    for index in range(early_count):
        unit(index, 0, True)
        ship(index, 0, 2)

    def pass_on(g, carry):
        share_copy(g, 2).wait_recv()
        forward_copy(g).start()
        return carry

    lax.fori_loop(0, groups, pass_on, 0)

    def passed(g, carry):
        forward_copy(g).wait_recv()
        return carry

    lax.fori_loop(0, groups, passed, 0)
    for index in range(early_count):
        unit(index, half, False)
        ship(index, 2, 2)

    late_indices = list(range(early_count, outer))
    if late_indices:
        r.acc[...] = jnp.zeros_like(r.acc)

        def late_step(step, carry):
            for slot, index in enumerate(late_indices):
                block = block_at(index)
                arrive(block, step)
                r.acc[slot] += product(block, step, 0, 2 * half)
            return carry

        lax.fori_loop(0, STEPS, late_step, 0)
        for slot, index in enumerate(late_indices):
            r.terms[index] = r.acc[slot].astype(dtype)
            ship(index, 2, 2)
            ship(index, 0, 2)

    for position in range(count):
        for which in range(heads):
            local_one = jnp.logical_and(which == head, lax.rem(position, INNER) == inner)

            @pl.when(jnp.logical_not(local_one))
            def _(which=which, position=position):
                remote(
                    r.terms.at[0, pl.ds(0, rows)],
                    r.landed.at[which, position],
                    r.term_send.at[0, 0, 0],
                    r.term_recv.at[which, position],
                    (seq, head),
                ).wait_recv()

    for position in range(count):
        total = r.landed[0, position].astype(jnp.float32)
        for which in range(1, heads):
            total = total + r.landed[which, position].astype(jnp.float32)
        r.out[:, position * tile : (position + 1) * tile] = total.astype(dtype)

    @pl.when(gives_halo)
    def _():
        for index in range(len(halos)):
            for which in range(heads):
                halo_copy(index, which, (seq + 1, which)).wait_send()

    for step in range(1, heads):
        dt_copy(step).wait_send()
    for index in range(1, INNER):
        log_copy(index).wait_send()

    def drain(g, carry):
        for kind in range(4):
            for step in range(1, heads):
                entry_copy(kind, g, step).wait_send()
        for index in range(1, INNER):
            piece_copy(g, index).wait_send()
            start_copy(g, index).wait_send()

        @pl.when(level < outer - 1)
        def _():
            chain_copy(g, seq).wait_send()

        share_copy(g, 1).wait_send()
        share_copy(g, 2).wait_send()
        forward_copy(g).wait_send()
        return carry

    lax.fori_loop(0, groups, drain, 0)
    if passes:

        def drain_weight(item, carry):
            which = lax.div(item, CHUNKS)
            chunk = lax.rem(item, CHUNKS)
            weight_item(1, which, chunk, "wait")
            weight_item(-1, which, chunk, "wait")
            return carry

        lax.fori_loop(0, passes * CHUNKS, drain_weight, 0)
    for index in range(outer):
        for mate in range(INNER):
            for which in range(heads):
                if mate == 0:

                    @pl.when(head != which)
                    def _(index=index, which=which):
                        result_copy(index, 0, which).wait_send()

                else:
                    result_copy(index, mate, which).wait_send()


def per_device(
    x_proj,
    z_proj,
    b_proj,
    c_proj,
    dt_raw,
    dt_bias,
    a_log,
    d_skip,
    conv_x,
    conv_bias_x,
    conv_bc,
    conv_bias_bc,
    norm_weight,
    out_weight,
):
    count = lax.axis_size("seq")
    heads = lax.axis_size("head")
    outer = count // INNER
    rows = x_proj.shape[0]
    tokens = rows * heads
    cols = x_proj.shape[1] // heads
    groups = b_proj.shape[1] // heads // STATE
    width = cols // groups
    local_heads = dt_bias.shape[0]
    blocks = tokens // SPAN
    part = width // INNER
    depth, tile = out_weight.shape
    passes = max(relay_passes(outer), 1)
    late = max(outer - (outer + 1) // 2, 1)
    dtype = x_proj.dtype
    f32 = jnp.float32
    vmem = pl.BlockSpec(memory_space=pltpu.VMEM)
    smem = pl.BlockSpec(memory_space=pltpu.SMEM)
    hbm = pl.BlockSpec(memory_space=pl.ANY)
    dma = pltpu.SemaphoreType.DMA
    inputs = {
        "x_in": (x_proj, hbm),
        "z_in": (z_proj, hbm),
        "b_in": (b_proj, hbm),
        "c_in": (c_proj, hbm),
        "dt_in": (dt_raw, hbm),
        "w_in": (out_weight, hbm),
        "dt_bias": (dt_bias[None], vmem),
        "a_log": (a_log[None], vmem),
        "skip": (d_skip, smem),
        "conv_x": (conv_x, vmem),
        "bias_x": (conv_bias_x[None], vmem),
        "conv_bc": (conv_bc, vmem),
        "bias_bc": (conv_bias_bc, vmem),
        "gain": (norm_weight[None], vmem),
    }
    scratch = {
        "x_buf": pltpu.VMEM((groups, tokens, width), dtype),
        "z_buf": pltpu.VMEM((groups, tokens, width), dtype),
        "b_buf": pltpu.VMEM((groups, tokens, STATE), dtype),
        "c_buf": pltpu.VMEM((groups, tokens, STATE), dtype),
        "dt_buf": pltpu.VMEM((tokens, dt_raw.shape[1]), dtype),
        "x_halo": pltpu.VMEM((HALO, cols), dtype),
        "b_halo": pltpu.VMEM((HALO, groups * STATE), dtype),
        "c_halo": pltpu.VMEM((HALO, groups * STATE), dtype),
        "wv": pltpu.VMEM((outer, depth, tile), dtype),
        "params": pltpu.VMEM((LANES, LANES), f32),
        "dt_t": pltpu.VMEM((dt_raw.shape[1], SPAN), f32),
        "step_t": pltpu.VMEM((local_heads, tokens), f32),
        "cum_t": pltpu.VMEM((local_heads, tokens), f32),
        "cum_pad": pltpu.VMEM((LANES, SPAN), f32),
        "cum_c": pltpu.VMEM((groups, tokens, LANES), f32),
        "log_out": pltpu.VMEM((8, LANES), f32),
        "log_in": pltpu.VMEM((INNER, 8, LANES), f32),
        "x_pad": pltpu.VMEM((tokens + 8, width), f32),
        "bc_pad": pltpu.VMEM((tokens + 8, STATE), f32),
        "x_t": pltpu.VMEM((width, SPAN), f32),
        "x_w": pltpu.VMEM((width, SPAN), dtype),
        "c_conv": pltpu.VMEM((groups, tokens, STATE), dtype),
        "y_t": pltpu.VMEM((groups, blocks, width, SPAN), f32),
        "pieces": pltpu.VMEM((groups, max(blocks - 1, 1), width, STATE), f32),
        "final": pltpu.VMEM((width, STATE), f32),
        "running": pltpu.VMEM((width, STATE), f32),
        "final_out": pltpu.VMEM((groups, width, STATE), dtype),
        "piece_in": pltpu.VMEM((groups, INNER, part, STATE), dtype),
        "chain_in": pltpu.VMEM((groups, part, STATE), dtype),
        "chain_out": pltpu.VMEM((groups, part, STATE), dtype),
        "start_out": pltpu.VMEM((groups, INNER, part, STATE), dtype),
        "start_in": pltpu.VMEM((groups, width, STATE), dtype),
        "a_buf": pltpu.VMEM((groups, INNER * tokens, width), dtype),
        "acc": pltpu.VMEM((late, INNER * tokens, tile), f32),
        "terms": pltpu.VMEM((outer, INNER * tokens, tile), dtype),
        "landed": pltpu.VMEM((heads, count, rows, tile), dtype),
        "entry_send": dma((4, heads, groups)),
        "entry_recv": dma((4, heads, groups)),
        "own_sems": dma((4, groups)),
        "misc_sems": dma((2,)),
        "dt_send": dma((heads,)),
        "dt_recv": dma((heads,)),
        "halo_send": dma((3, heads)),
        "halo_recv": dma((3,)),
        "weight_send": dma((2, passes, CHUNKS)),
        "weight_recv": dma((outer, CHUNKS)),
        "log_send": dma((INNER,)),
        "log_recv": dma((INNER,)),
        "piece_send": dma((groups, INNER)),
        "piece_recv": dma((groups, INNER)),
        "chain_send": dma((groups,)),
        "chain_recv": dma((groups,)),
        "start_send": dma((groups, INNER)),
        "start_recv": dma((groups, INNER)),
        "share_send": dma((groups, INNER)),
        "share_recv": dma((groups, INNER)),
        "term_send": dma((outer, INNER, heads)),
        "term_recv": dma((heads, count)),
    }
    names = list(inputs) + ["out"] + list(scratch)
    return pl.pallas_call(
        functools.partial(mixer_kernel, count, heads, names),
        out_shape=jax.ShapeDtypeStruct((rows, count * tile), dtype),
        in_specs=[spec for _, spec in inputs.values()],
        out_specs=vmem,
        scratch_shapes=list(scratch.values()),
        compiler_params=pltpu.CompilerParams(
            collective_id=0, has_side_effects=True, vmem_limit_bytes=60 * 1024 * 1024
        ),
        name="mixer",
    )(*[value for value, _ in inputs.values()])


def solution(mesh):
    in_specs = (
        P(("seq", "head"), None),
        P(("seq", "head"), None),
        P(("seq", "head"), None),
        P(("seq", "head"), None),
        P(("seq", "head"), None),
        P("head"),
        P("head"),
        P("head"),
        P(None, "head"),
        P("head"),
        P(None, None, "head"),
        P(None, "head"),
        P("head"),
        P("head", "seq"),
    )
    out_specs = P(("seq", "head"), None)
    return jax.shard_map(
        per_device, mesh=mesh, in_specs=in_specs, out_specs=out_specs, check_vma=False
    )
```

```python
import functools
import types

import jax
import jax.numpy as jnp
from jax import lax
from jax.experimental import pallas as pl
from jax.experimental.pallas import tpu as pltpu
from jax.sharding import PartitionSpec as P

HEAD_DIM = 64
STATE = 128
SPAN = 128
HALO = 16
INNER = 4
CHUNKS = 16
STEPS = 8
OPENING = 2
RELAYED = 4
FIRST = 4
LATE_GROUP = 3
LANES = 128
NT = (((1,), (1,)), ((), ()))
MESH = pl.DeviceIdType.MESH


def relay_passes(outer):
    passes = 0
    for level in range(outer):
        room = outer - 1 - level
        behind = level // 2 + 1
        if room >= 1:
            passes = max(passes, behind * min(room, 2))
    return passes


def column_orders(outer):
    edge = list(range(outer))
    if outer < 4:
        return edge, edge
    first = [0, 2, outer - 1, 1]
    return edge, first + [offset for offset in edge if offset not in first]


def conv_silu(value, halo, taps_of, bias, padded, dtype):
    tokens = value.shape[0]
    padded[0:8, :] = halo.astype(jnp.float32)
    padded[8 : 8 + tokens, :] = value.astype(jnp.float32)
    total = bias + jnp.zeros(value.shape, jnp.float32)
    taps = len(taps_of)
    for offset in range(taps):
        low = 8 - (taps - 1) + offset
        total = total + taps_of[offset] * padded[low : low + tokens, :]
    return (total / (1.0 + jnp.exp(-total))).astype(dtype)


def mixer_kernel(count, heads, names, *refs):
    r = types.SimpleNamespace(**dict(zip(names, refs)))
    seq = lax.axis_index("seq")
    head = lax.axis_index("head")
    outer = count // INNER
    inner = lax.rem(seq, INNER)
    level = lax.div(seq, INNER)
    rows = r.x_in.shape[0]
    tokens = rows * heads
    groups, _, width = r.x_buf.shape
    per = width // HEAD_DIM
    blocks = tokens // SPAN
    local_heads = groups * per
    part = width // INNER
    part_heads = part // HEAD_DIM
    depth = r.wv.shape[1]
    tile = r.wv.shape[2]
    chunk_rows = depth // CHUNKS
    step_rows = depth // STEPS
    passes = relay_passes(outer)
    taps = r.conv_x.shape[0]
    dtype = r.x_buf.dtype

    near = seq + 1 - 2 * lax.rem(seq, 2)
    side = seq + 2 - 4 * lax.rem(lax.div(seq, 2), 2)
    cross = near + side - seq
    mates = (seq, near, side, cross)
    inners = tuple(lax.rem(mate, INNER) for mate in mates)

    def remote(source, target, send, recv, device):
        return pltpu.make_async_remote_copy(
            src_ref=source,
            dst_ref=target,
            send_sem=send,
            recv_sem=recv,
            device_id=device,
            device_id_type=MESH,
        )

    def head_of(step):
        return lax.rem(head + step, heads)

    barrier = pltpu.get_barrier_semaphore()
    gives_halo = jnp.logical_and(head == heads - 1, seq < count - 1)
    takes_halo = seq > 0
    gives_out = jnp.logical_and(gives_halo, inner == INNER - 1)
    takes_out = jnp.logical_and(takes_halo, inner == 0)

    def greet(where, which):
        pl.semaphore_signal(barrier, inc=1, device_id=(where, which), device_id_type=MESH)

    for index, mate in enumerate(mates):
        for step in range(heads):
            if index or step:
                greet(mate, head_of(step))
    expected = jnp.int32(INNER * heads - 1)
    for sign in (1, -1):
        for distance in (1, 2):
            there = level + sign * distance
            exists = jnp.logical_and(there >= 0, there < outer)

            @pl.when(exists)
            def _(there=there):
                greet(there * INNER + inner, head)

            expected = expected + jnp.where(exists, 1, 0)

    @pl.when(gives_out)
    def _():
        for which in range(heads):
            greet(seq + 1, which)

    @pl.when(takes_out)
    def _():
        greet(seq - 1, heads - 1)

    expected = expected + jnp.where(gives_out, heads, 0) + jnp.where(takes_out, 1, 0)
    with jax.named_scope("greeting"):
        pl.semaphore_wait(barrier, expected)

    mine = pl.ds(pl.multiple_of(head * rows, 16), rows)
    plan = (
        (r.b_in, r.b_buf, STATE),
        (r.c_in, r.c_buf, STATE),
        (r.x_in, r.x_buf, width),
        (r.z_in, r.z_buf, width),
    )
    halos = ((r.x_in, r.x_halo), (r.b_in, r.b_halo), (r.c_in, r.c_halo))

    def halo_copy(index, which, device):
        source, target = halos[index]
        size = target.shape[1]
        return remote(
            source.at[pl.ds(rows - HALO, HALO), pl.ds(which * size, size)],
            target,
            r.halo_send.at[index, which],
            r.halo_recv.at[index],
            device,
        )

    def entry_view(kind, which, g):
        source, target, size = plan[kind]
        low = pl.multiple_of((which * groups + g) * size, LANES)
        return source.at[:, pl.ds(low, size)], target.at[g, mine]

    def entry_copy(kind, g, step):
        source, target = entry_view(kind, head_of(step), g)
        return remote(
            source,
            target,
            r.entry_send.at[kind, step, g],
            r.entry_recv.at[kind, step, g],
            (seq, head_of(step)),
        )

    def own_copy(kind, g):
        source, target = entry_view(kind, head, g)
        return pltpu.make_async_copy(source, target, r.own_sems.at[kind, g])

    def dt_copy(step):
        return remote(
            r.dt_in,
            r.dt_buf.at[mine],
            r.dt_send.at[step],
            r.dt_recv.at[step],
            (seq, head_of(step)),
        )

    own_dt = pltpu.make_async_copy(r.dt_in, r.dt_buf.at[mine], r.misc_sems.at[0])
    own_weight = pltpu.make_async_copy(r.w_in, r.wv.at[level], r.misc_sems.at[1])

    own_dt.start()
    for step in range(1, heads):
        dt_copy(step).start()
    own_weight.start()

    @pl.when(gives_halo)
    def _():
        for index in range(len(halos)):
            for which in range(heads):
                halo_copy(index, which, (seq + 1, which)).start()

    for g in range(groups):
        for kind in range(3):
            own_copy(kind, g).start()
            for step in range(1, heads):
                entry_copy(kind, g, step).start()
    for g in range(groups):
        own_copy(3, g).start()
        for step in range(1, heads):
            entry_copy(3, g, step).start()

    def weight_item(sign, which, chunk, kinds):
        room = outer - 1 - level if sign > 0 else level
        behind = lax.div(level if sign > 0 else outer - 1 - level, 2)
        far = room >= 2
        hops = jnp.where(far, lax.div(which, 2), which)
        distance = jnp.where(far, 2 - lax.rem(which, 2), 1)
        exists = jnp.logical_and(room >= 1, hops <= behind)
        edge = level == 0 if sign > 0 else level == outer - 1
        if kinds is not None:
            between = jnp.logical_and(far, jnp.logical_not(edge))
            chosen = jnp.bool_(False)
            if "edge" in kinds:
                chosen = jnp.logical_or(chosen, jnp.logical_and(far, edge))
            if "last" in kinds:
                chosen = jnp.logical_or(chosen, jnp.logical_not(far))
            if ("up" if sign > 0 else "down") in kinds:
                chosen = jnp.logical_or(chosen, between)
            exists = jnp.logical_and(exists, chosen)
        block = level - sign * 2 * hops
        target = (level + sign * distance) * INNER + inner
        view = r.wv.at[block, pl.ds(pl.multiple_of(chunk * chunk_rows, 16), chunk_rows)]
        copy = remote(
            view,
            view,
            r.weight_send.at[0 if sign > 0 else 1, which],
            r.weight_recv.at[block, chunk],
            (target, head),
        )
        if kinds is None:

            @pl.when(exists)
            def _():
                whole = r.wv.at[level]
                remote(
                    whole,
                    whole,
                    r.weight_send.at[0 if sign > 0 else 1, which],
                    r.weight_recv.at[level, 0],
                    (target, head),
                ).wait_send()

            return
        fresh = jnp.logical_or(jnp.logical_not(far), distance == 2)
        relayed = jnp.logical_and(jnp.logical_and(exists, hops >= 1), fresh)

        @pl.when(relayed)
        def _():
            copy.wait_recv()

        @pl.when(exists)
        def _():
            copy.start()

    def weight_pass(which, kinds, low=0, high=CHUNKS):
        def body(chunk, carry):
            if set(kinds) != {"down"}:
                weight_item(1, which, chunk, kinds)
            if set(kinds) != {"up"}:
                weight_item(-1, which, chunk, kinds)
            return carry

        lax.fori_loop(low, high, body, 0)

    def weight_arrived(block, chunk):
        below = block < level
        apart = jnp.where(below, level - block, block - level)
        room = jnp.where(below, outer - 1 - level, level)
        relayed = jnp.logical_and(lax.rem(apart, 2) == 0, room >= 1)

        @pl.when(jnp.logical_and(apart > 0, jnp.logical_not(relayed)))
        def _():
            view = r.wv.at[block, pl.ds(pl.multiple_of(chunk * chunk_rows, 16), chunk_rows)]
            remote(
                view,
                view,
                r.weight_send.at[0, 0],
                r.weight_recv.at[block, chunk],
                (seq, head),
            ).wait_recv()

    own_weight.wait()
    if passes > 1:
        weight_pass(1, ("edge", "up"), 0, OPENING)
    if passes:
        weight_pass(0, ("edge", "last", "down"))

    r.params[...] = jnp.zeros_like(r.params)
    r.params[0:1, 0:local_heads] = r.dt_bias[...]
    r.params[1:2, 0:local_heads] = r.a_log[...]
    columns = r.params[...].T
    bias = columns[0:local_heads, 0:1]
    coeff = -jnp.exp(columns[0:local_heads, 1:2])
    own_dt.wait()
    for step in range(1, heads):
        dt_copy(step).wait_recv()
    early = lax.broadcasted_iota(jnp.int32, (SPAN, SPAN), 0)
    late = lax.broadcasted_iota(jnp.int32, (SPAN, SPAN), 1)
    prefix_ones = jnp.where(early <= late, 1.0, 0.0).astype(jnp.float32)
    r.cum_pad[...] = jnp.zeros_like(r.cum_pad)
    log_total = jnp.zeros((1, LANES), jnp.float32)
    for block in range(blocks):
        span = slice(block * SPAN, (block + 1) * SPAN)
        r.dt_t[...] = r.dt_buf[span, :].astype(jnp.float32).T
        raw = r.dt_t[pl.ds(pl.multiple_of(head * local_heads, 8), local_heads), :] + bias
        step_size = jnp.maximum(raw, 0.0) + jnp.log1p(jnp.exp(-jnp.abs(raw)))
        r.step_t[:, span] = step_size
        summed = jnp.dot(
            coeff * step_size,
            prefix_ones,
            preferred_element_type=jnp.float32,
            precision=lax.Precision.HIGHEST,
        )
        r.cum_t[:, span] = summed
        r.cum_pad[0:local_heads, :] = summed
        by_token = r.cum_pad[...].T
        log_total = log_total + by_token[SPAN - 1 : SPAN, :]
        for g in range(groups):
            shift = (LANES - g * per) % LANES
            r.cum_c[g, span, :] = pltpu.roll(by_token, shift, 1) if shift else by_token
    logs = jnp.broadcast_to(log_total, (8, LANES))
    r.log_out[...] = logs
    r.log_in[inner] = logs

    def log_copy(index):
        return remote(
            r.log_out,
            r.log_in.at[inner],
            r.log_send.at[index],
            r.log_recv.at[index],
            (mates[index], head),
        )

    for index in range(1, INNER):
        log_copy(index).start()

    @pl.when(jnp.logical_not(takes_halo))
    def _():
        for _, target in halos:
            target[...] = jnp.zeros_like(target)

    @pl.when(takes_halo)
    def _():
        for index in range(len(halos)):
            halo_copy(index, 0, (seq, head)).wait_recv()

    @pl.when(level == 0)
    def _():
        r.chain_in[...] = jnp.zeros_like(r.chain_in)

    causal = early >= late

    def piece_copy(g, index):
        low = pl.multiple_of(inners[index] * part, 16)
        return remote(
            r.final_out.at[g, pl.ds(low, part)],
            r.piece_in.at[g, inner],
            r.piece_send.at[g, index],
            r.piece_recv.at[g, index],
            (mates[index], head),
        )

    def local(g, carry):
        with jax.named_scope("local_wait"):
            for kind in range(3):
                own_copy(kind, g).wait()
                for step in range(1, heads):
                    entry_copy(kind, g, step).wait_recv()
        wide = pl.ds(pl.multiple_of(g * width, LANES), width)
        slim = pl.ds(pl.multiple_of(g * STATE, LANES), STATE)
        x_conv = conv_silu(
            r.x_buf[g],
            r.x_halo[HALO - 8 : HALO, wide],
            [r.conv_x[tap : tap + 1, wide] for tap in range(taps)],
            r.bias_x[:, wide],
            r.x_pad,
            dtype,
        )
        b_conv = conv_silu(
            r.b_buf[g],
            r.b_halo[HALO - 8 : HALO, slim],
            [r.conv_bc[tap, 0:1, slim] for tap in range(taps)],
            r.bias_bc[0:1, slim],
            r.bc_pad,
            dtype,
        )
        c_conv = conv_silu(
            r.c_buf[g],
            r.c_halo[HALO - 8 : HALO, slim],
            [r.conv_bc[tap, 1:2, slim] for tap in range(taps)],
            r.bias_bc[1:2, slim],
            r.bc_pad,
            dtype,
        )
        r.c_conv[g] = c_conv
        own_heads = pl.ds(pl.multiple_of(g * per, 8), per)
        for block in range(blocks):
            low = block * SPAN
            b_blk = b_conv[low : low + SPAN]
            c_blk = c_conv[low : low + SPAN]
            r.x_t[...] = x_conv[low : low + SPAN].astype(jnp.float32).T
            scores = lax.dot_general(c_blk, b_blk, NT, preferred_element_type=jnp.float32)
            cum_rows = r.cum_t[own_heads, low : low + SPAN]
            step_all = r.step_t[own_heads, low : low + SPAN]
            for index in range(per):
                lines = pl.ds(index * HEAD_DIM, HEAD_DIM)
                column = r.cum_c[g, low : low + SPAN, index : index + 1]
                row = cum_rows[index : index + 1, :]
                step = step_all[index : index + 1, :]
                total = row[:, SPAN - 1 : SPAN]
                decays = jnp.exp(jnp.where(causal, column - row, -jnp.inf))
                mix = (decays * step * scores).astype(dtype)
                x_head = r.x_t[lines, :]
                product = lax.dot_general(
                    x_head.astype(dtype), mix, NT, preferred_element_type=jnp.float32
                )
                r.y_t[g, block, lines, :] = product + r.skip[g * per + index] * x_head
                r.x_w[lines, :] = (x_head * (step * jnp.exp(total - row))).astype(dtype)
            piece = jnp.dot(r.x_w[...], b_blk, preferred_element_type=jnp.float32)
            if block < blocks - 1:
                r.pieces[g, block] = piece
            if block == 0:
                r.final[...] = piece
            else:
                r.running[...] = piece
                for index in range(per):
                    lines = pl.ds(index * HEAD_DIM, HEAD_DIM)
                    decay = jnp.exp(cum_rows[index : index + 1, SPAN - 1 : SPAN])
                    r.final[lines, :] = decay * r.final[lines, :] + r.running[lines, :]
        r.final_out[g] = r.final[...].astype(dtype)
        for index in range(1, INNER):
            piece_copy(g, index).start()
        own_part = pl.ds(pl.multiple_of(inner * part, 16), part)
        r.piece_in[g, inner] = r.final_out[g, own_part, :]
        return carry

    with jax.named_scope("local_all"):
        lax.fori_loop(0, groups, local, 0)
    if passes > 1:
        weight_pass(1, ("last",), 0, RELAYED)

    def chain_copy(g, where):
        return remote(
            r.chain_out.at[g],
            r.chain_in.at[g],
            r.chain_send.at[g],
            r.chain_recv.at[g],
            (where, head),
        )

    def start_copy(g, index):
        low = pl.multiple_of(inner * part, 16)
        return remote(
            r.start_out.at[g, inners[index]],
            r.start_in.at[g, pl.ds(low, part)],
            r.start_send.at[g, index],
            r.start_recv.at[g, index],
            (mates[index], head),
        )

    for index in range(1, INNER):
        log_copy(index).wait_recv()

    def carry_step(g, carry):
        with jax.named_scope("carry_wait"):
            for index in range(1, INNER):
                piece_copy(g, index).wait_recv()

            @pl.when(level > 0)
            def _():
                chain_copy(g, seq).wait_recv()

        first = g * per + inner * part_heads
        state = [
            r.chain_in[g, index * HEAD_DIM : (index + 1) * HEAD_DIM, :].astype(jnp.float32)
            for index in range(part_heads)
        ]
        for position in range(INNER):
            decays = jnp.exp(pltpu.roll(r.log_in[position], lax.rem(LANES - first, LANES), 1))
            for index in range(part_heads):
                lines = slice(index * HEAD_DIM, (index + 1) * HEAD_DIM)
                r.start_out[g, position, lines, :] = state[index].astype(dtype)
                piece = r.piece_in[g, position, lines, :].astype(jnp.float32)
                state[index] = decays[0:1, index : index + 1] * state[index] + piece
        for index in range(part_heads):
            r.chain_out[g, index * HEAD_DIM : (index + 1) * HEAD_DIM, :] = state[index].astype(
                dtype
            )

        @pl.when(level < outer - 1)
        def _():
            chain_copy(g, seq + INNER).start()

        for index in range(1, INNER):
            start_copy(g, index).start()
        own_part = pl.ds(pl.multiple_of(inner * part, 16), part)
        r.start_in[g, own_part, :] = r.start_out[g, inner]
        return carry

    with jax.named_scope("carry_all"):
        lax.fori_loop(0, groups, carry_step, 0)

    def chain_left(g, carry):
        @pl.when(level < outer - 1)
        def _():
            chain_copy(g, seq).wait_send()

        return carry

    with jax.named_scope("chain_left"):
        lax.fori_loop(0, groups, chain_left, 0)

    if passes > 1:
        with jax.named_scope("pass_one_early"):
            weight_pass(1, ("edge",), OPENING)
            weight_pass(1, ("last",), RELAYED)
            weight_pass(1, ("down",))
            weight_pass(1, ("up",), OPENING, OPENING + FIRST)

    def share_copy(g, index):
        target = r.a_buf.at[g, pl.ds(index * tokens, tokens)]
        return remote(
            r.a_buf.at[g, pl.ds(0, tokens)],
            target,
            r.share_send.at[g, index],
            r.share_recv.at[g, index],
            (mates[index], head),
        )

    def forward_copy(g):
        return remote(
            r.a_buf.at[g, pl.ds(2 * tokens, tokens)],
            r.a_buf.at[g, pl.ds(3 * tokens, tokens)],
            r.share_send.at[g, 3],
            r.share_recv.at[g, 3],
            (near, head),
        )

    def norm_step(g, carry):
        with jax.named_scope("norm_wait"):
            for index in range(1, INNER):
                start_copy(g, index).wait_recv()
            own_copy(3, g).wait()
            for step in range(1, heads):
                entry_copy(3, g, step).wait_recv()
        wide = pl.ds(pl.multiple_of(g * width, LANES), width)
        own_heads = pl.ds(pl.multiple_of(g * per, 8), per)
        r.running[...] = r.start_in[g].astype(jnp.float32)
        for block in range(blocks):
            low = block * SPAN
            c_blk = r.c_conv[g, low : low + SPAN, :]
            r.x_t[...] = lax.dot_general(
                r.running[...].astype(dtype), c_blk, NT, preferred_element_type=jnp.float32
            )
            grown = jnp.exp(r.cum_t[own_heads, low : low + SPAN])
            for index in range(per):
                lines = pl.ds(index * HEAD_DIM, HEAD_DIM)
                row = grown[index : index + 1, :]
                r.x_t[lines, :] = r.y_t[g, block, lines, :] + r.x_t[lines, :] * row
                if block < blocks - 1:
                    r.running[lines, :] = (
                        row[:, SPAN - 1 : SPAN] * r.running[lines, :]
                        + r.pieces[g, block, lines, :]
                    )
            gate = r.z_buf[g, low : low + SPAN, :].astype(jnp.float32)
            gated = r.x_t[...].T * (gate / (1.0 + jnp.exp(-gate)))
            mean = jnp.sum(gated * gated, axis=-1, keepdims=True) * (1.0 / width)
            normed = gated * lax.rsqrt(mean + 1.0)
            r.a_buf[g, low : low + SPAN, :] = (normed * r.gain[:, wide]).astype(dtype)
        share_copy(g, 2).start()
        share_copy(g, 1).start()

        if passes:

            @pl.when(g == min(LATE_GROUP, groups - 1))
            def _():
                weight_pass(0, ("up",))

        return carry

    with jax.named_scope("norm_all"):
        lax.fori_loop(0, groups, norm_step, 0)

    if passes > 1:
        with jax.named_scope("pass_one_late"):
            weight_pass(1, ("up",), OPENING + FIRST)

    def later_pass(which, carry):
        weight_pass(which, ("edge", "last", "up", "down"))
        return carry

    if passes > 2:
        lax.fori_loop(2, passes, later_pass, 0)

    edge_order, inner_order = column_orders(outer)
    early_count = min(2, outer)
    at_edge = jnp.logical_or(level == 0, level == outer - 1)
    direction = jnp.where(level < (outer + 1) // 2, 1, -1)

    def block_at(index):
        offset = jnp.where(at_edge, edge_order[index], inner_order[index])
        return lax.rem(level + direction * offset + outer, outer)

    steps_per_group = width // step_rows

    def product(block, step, low, size):
        g = lax.div(step, steps_per_group)
        off = pl.multiple_of(lax.rem(step, steps_per_group) * step_rows, LANES)
        down = pl.multiple_of(step * step_rows, 16)
        return jnp.dot(
            r.a_buf[g, low : low + size, pl.ds(off, step_rows)],
            r.wv[block, pl.ds(down, step_rows), :],
            preferred_element_type=jnp.float32,
        )

    per_step = CHUNKS // STEPS

    def arrive(block, step):
        for extra in range(per_step):
            weight_arrived(block, step * per_step + extra)

    def result_copy(index, mate, which):
        low = pl.multiple_of(mate * tokens + which * rows, 16)
        return remote(
            r.terms.at[index, pl.ds(low, rows)],
            r.landed.at[head, block_at(index) * INNER + inner],
            r.term_send.at[index],
            r.term_recv.at[head, block_at(index) * INNER + inner],
            (mates[mate], which),
        )

    def ship(index, low_mate, mate_count):
        for mate in range(low_mate, low_mate + mate_count):
            for which in range(heads):
                if mate == 0:

                    @pl.when(head != which)
                    def _(mate=mate, which=which):
                        result_copy(index, mate, which).start()

                else:
                    result_copy(index, mate, which).start()
        if low_mate == 0:
            own_rows = pl.ds(pl.multiple_of(head * rows, 16), rows)
            r.landed[head, block_at(index) * INNER + inner] = r.terms[index, own_rows, :]

    half = 2 * tokens

    def unit(index, low, size, waits):
        block = block_at(index)
        r.acc[0:size, :] = jnp.zeros((size, tile), jnp.float32)

        def body(step, carry):
            if waits:
                arrive(block, step)
            r.acc[0:size, :] += product(block, step, low, size)
            return carry

        lax.fori_loop(0, STEPS, body, 0)
        r.terms[index, low : low + size, :] = r.acc[0:size, :].astype(dtype)

    for g in range(groups):
        share_copy(g, 1).wait_recv()
    for index in range(early_count):
        with jax.named_scope("early_zero"):
            unit(index, 0, half, True)
            ship(index, 0, 2)

    def pass_on(g, carry):
        share_copy(g, 2).wait_recv()
        forward_copy(g).start()
        return carry

    with jax.named_scope("pass_on"):
        lax.fori_loop(0, groups, pass_on, 0)

    def passed(g, carry):
        forward_copy(g).wait_recv()
        return carry

    with jax.named_scope("passed"):
        lax.fori_loop(0, groups, passed, 0)
    for index in range(early_count):
        with jax.named_scope("early_one"):
            unit(index, half, half, False)
            ship(index, 2, 2)

    @pl.when(gives_halo)
    def _():
        for index in range(len(halos)):
            for which in range(heads):
                halo_copy(index, which, (seq + 1, which)).wait_send()

    for step in range(1, heads):
        dt_copy(step).wait_send()
    for index in range(1, INNER):
        log_copy(index).wait_send()

    def drain(g, carry):
        for kind in range(4):
            for step in range(1, heads):
                entry_copy(kind, g, step).wait_send()
        for index in range(1, INNER):
            piece_copy(g, index).wait_send()
            start_copy(g, index).wait_send()
        share_copy(g, 1).wait_send()
        share_copy(g, 2).wait_send()
        forward_copy(g).wait_send()
        return carry

    lax.fori_loop(0, groups, drain, 0)

    def results_of(index):
        for mate in range(INNER):
            for which in range(heads):
                position = block_at(index) * INNER + mate
                local_one = jnp.logical_and(which == head, mate == inner)

                @pl.when(jnp.logical_not(local_one))
                def _(which=which, position=position):
                    remote(
                        r.terms.at[0, pl.ds(0, rows)],
                        r.landed.at[which, position],
                        r.term_send.at[0],
                        r.term_recv.at[which, position],
                        (near, head),
                    ).wait_recv()

    for index in range(early_count, outer):
        if index == outer - 1:
            with jax.named_scope("results_early"):
                for before in range(index):
                    results_of(before)
        with jax.named_scope("late"):
            unit(index, 0, 2 * half, True)
            ship(index, 2, 2)
            ship(index, 0, 2)

    with jax.named_scope("result_wait"):
        for index in range(0 if outer == early_count else outer - 1, outer):
            results_of(index)

    with jax.named_scope("assembly"):
        for position in range(count):
            total = r.landed[0, position].astype(jnp.float32)
            for which in range(1, heads):
                total = total + r.landed[which, position].astype(jnp.float32)
            r.out[:, position * tile : (position + 1) * tile] = total.astype(dtype)

    if passes:

        def drain_weight(which, carry):
            weight_item(1, which, 0, None)
            weight_item(-1, which, 0, None)
            return carry

        lax.fori_loop(0, passes, drain_weight, 0)
    for index in range(outer):
        sent = pl.ds(0, (INNER * heads - 1) * rows)
        remote(
            r.terms.at[index, sent],
            r.terms.at[index, sent],
            r.term_send.at[index],
            r.term_recv.at[0, 0],
            (near, head),
        ).wait_send()


def per_device(
    x_proj,
    z_proj,
    b_proj,
    c_proj,
    dt_raw,
    dt_bias,
    a_log,
    d_skip,
    conv_x,
    conv_bias_x,
    conv_bc,
    conv_bias_bc,
    norm_weight,
    out_weight,
):
    count = lax.axis_size("seq")
    heads = lax.axis_size("head")
    outer = count // INNER
    rows = x_proj.shape[0]
    tokens = rows * heads
    cols = x_proj.shape[1] // heads
    groups = b_proj.shape[1] // heads // STATE
    width = cols // groups
    local_heads = dt_bias.shape[0]
    blocks = tokens // SPAN
    part = width // INNER
    depth, tile = out_weight.shape
    passes = max(relay_passes(outer), 1)
    dtype = x_proj.dtype
    f32 = jnp.float32
    vmem = pl.BlockSpec(memory_space=pltpu.VMEM)
    smem = pl.BlockSpec(memory_space=pltpu.SMEM)
    hbm = pl.BlockSpec(memory_space=pl.ANY)
    dma = pltpu.SemaphoreType.DMA
    inputs = {
        "x_in": (x_proj, hbm),
        "z_in": (z_proj, hbm),
        "b_in": (b_proj, hbm),
        "c_in": (c_proj, hbm),
        "dt_in": (dt_raw, hbm),
        "w_in": (out_weight, hbm),
        "dt_bias": (dt_bias[None], vmem),
        "a_log": (a_log[None], vmem),
        "skip": (d_skip, smem),
        "conv_x": (conv_x, vmem),
        "bias_x": (conv_bias_x[None], vmem),
        "conv_bc": (conv_bc, vmem),
        "bias_bc": (conv_bias_bc, vmem),
        "gain": (norm_weight[None], vmem),
    }
    scratch = {
        "x_buf": pltpu.VMEM((groups, tokens, width), dtype),
        "z_buf": pltpu.VMEM((groups, tokens, width), dtype),
        "b_buf": pltpu.VMEM((groups, tokens, STATE), dtype),
        "c_buf": pltpu.VMEM((groups, tokens, STATE), dtype),
        "dt_buf": pltpu.VMEM((tokens, dt_raw.shape[1]), dtype),
        "x_halo": pltpu.VMEM((HALO, cols), dtype),
        "b_halo": pltpu.VMEM((HALO, groups * STATE), dtype),
        "c_halo": pltpu.VMEM((HALO, groups * STATE), dtype),
        "wv": pltpu.VMEM((outer, depth, tile), dtype),
        "params": pltpu.VMEM((LANES, LANES), f32),
        "dt_t": pltpu.VMEM((dt_raw.shape[1], SPAN), f32),
        "step_t": pltpu.VMEM((local_heads, tokens), f32),
        "cum_t": pltpu.VMEM((local_heads, tokens), f32),
        "cum_pad": pltpu.VMEM((LANES, SPAN), f32),
        "cum_c": pltpu.VMEM((groups, tokens, LANES), f32),
        "log_out": pltpu.VMEM((8, LANES), f32),
        "log_in": pltpu.VMEM((INNER, 8, LANES), f32),
        "x_pad": pltpu.VMEM((tokens + 8, width), f32),
        "bc_pad": pltpu.VMEM((tokens + 8, STATE), f32),
        "x_t": pltpu.VMEM((width, SPAN), f32),
        "x_w": pltpu.VMEM((width, SPAN), dtype),
        "c_conv": pltpu.VMEM((groups, tokens, STATE), dtype),
        "y_t": pltpu.VMEM((groups, blocks, width, SPAN), f32),
        "pieces": pltpu.VMEM((groups, max(blocks - 1, 1), width, STATE), f32),
        "final": pltpu.VMEM((width, STATE), f32),
        "running": pltpu.VMEM((width, STATE), f32),
        "final_out": pltpu.VMEM((groups, width, STATE), dtype),
        "piece_in": pltpu.VMEM((groups, INNER, part, STATE), dtype),
        "chain_in": pltpu.VMEM((groups, part, STATE), dtype),
        "chain_out": pltpu.VMEM((groups, part, STATE), dtype),
        "start_out": pltpu.VMEM((groups, INNER, part, STATE), dtype),
        "start_in": pltpu.VMEM((groups, width, STATE), dtype),
        "a_buf": pltpu.VMEM((groups, INNER * tokens, width), dtype),
        "acc": pltpu.VMEM((INNER * tokens, tile), f32),
        "terms": pltpu.VMEM((outer, INNER * tokens, tile), dtype),
        "landed": pltpu.VMEM((heads, count, rows, tile), dtype),
        "entry_send": dma((4, heads, groups)),
        "entry_recv": dma((4, heads, groups)),
        "own_sems": dma((4, groups)),
        "misc_sems": dma((2,)),
        "dt_send": dma((heads,)),
        "dt_recv": dma((heads,)),
        "halo_send": dma((3, heads)),
        "halo_recv": dma((3,)),
        "weight_send": dma((2, passes)),
        "weight_recv": dma((outer, CHUNKS)),
        "log_send": dma((INNER,)),
        "log_recv": dma((INNER,)),
        "piece_send": dma((groups, INNER)),
        "piece_recv": dma((groups, INNER)),
        "chain_send": dma((groups,)),
        "chain_recv": dma((groups,)),
        "start_send": dma((groups, INNER)),
        "start_recv": dma((groups, INNER)),
        "share_send": dma((groups, INNER)),
        "share_recv": dma((groups, INNER)),
        "term_send": dma((outer,)),
        "term_recv": dma((heads, count)),
    }
    names = list(inputs) + ["out"] + list(scratch)
    return pl.pallas_call(
        functools.partial(mixer_kernel, count, heads, names),
        out_shape=jax.ShapeDtypeStruct((rows, count * tile), dtype),
        in_specs=[spec for _, spec in inputs.values()],
        out_specs=vmem,
        scratch_shapes=list(scratch.values()),
        compiler_params=pltpu.CompilerParams(
            collective_id=0, has_side_effects=True, vmem_limit_bytes=60 * 1024 * 1024
        ),
        name="mixer",
    )(*[value for value, _ in inputs.values()])


def solution(mesh):
    in_specs = (
        P(("seq", "head"), None),
        P(("seq", "head"), None),
        P(("seq", "head"), None),
        P(("seq", "head"), None),
        P(("seq", "head"), None),
        P("head"),
        P("head"),
        P("head"),
        P(None, "head"),
        P("head"),
        P(None, None, "head"),
        P(None, "head"),
        P("head"),
        P("head", "seq"),
    )
    out_specs = P(("seq", "head"), None)
    return jax.shard_map(
        per_device, mesh=mesh, in_specs=in_specs, out_specs=out_specs, check_vma=False
    )
```

```python
import functools
import types

import jax
import jax.numpy as jnp
from jax import lax
from jax.experimental import pallas as pl
from jax.experimental.pallas import tpu as pltpu
from jax.sharding import PartitionSpec as P

HEAD_DIM = 64
STATE = 128
SPAN = 128
HALO = 16
INNER = 4
CHUNKS = 16
STEPS = 8
OPENING = 2
BEFORE = 12
RELAYED = 4
FIRST = 4
LATE_GROUP = 3
LANES = 128
NT = (((1,), (1,)), ((), ()))
MESH = pl.DeviceIdType.MESH


def relay_passes(outer):
    passes = 0
    for level in range(outer):
        room = outer - 1 - level
        behind = level // 2 + 1
        if room >= 1:
            passes = max(passes, behind * min(room, 2))
    return passes


def column_halves(tile):
    return 2 if tile % (2 * LANES) == 0 else 1


def column_orders(outer):
    edge = list(range(outer))
    if outer < 4:
        return edge, edge
    first = [0, 2, outer - 1, 1]
    return edge, first + [offset for offset in edge if offset not in first]


def conv_silu(value, halo, taps_of, bias, padded, dtype):
    tokens = value.shape[0]
    padded[0:8, :] = halo.astype(jnp.float32)
    padded[8 : 8 + tokens, :] = value.astype(jnp.float32)
    total = bias + jnp.zeros(value.shape, jnp.float32)
    taps = len(taps_of)
    for offset in range(taps):
        low = 8 - (taps - 1) + offset
        total = total + taps_of[offset] * padded[low : low + tokens, :]
    return (total / (1.0 + jnp.exp(-total))).astype(dtype)


def mixer_kernel(count, heads, names, *refs):
    r = types.SimpleNamespace(**dict(zip(names, refs)))
    seq = lax.axis_index("seq")
    head = lax.axis_index("head")
    outer = count // INNER
    inner = lax.rem(seq, INNER)
    level = lax.div(seq, INNER)
    rows = r.x_in.shape[0]
    tokens = rows * heads
    groups, _, width = r.x_buf.shape
    per = width // HEAD_DIM
    blocks = tokens // SPAN
    local_heads = groups * per
    part = width // INNER
    part_heads = part // HEAD_DIM
    depth = r.wv.shape[1]
    tile = r.wv.shape[2]
    halves = column_halves(tile)
    half_cols = tile // halves
    per_half = CHUNKS // halves
    chunk_rows = depth // per_half
    step_rows = depth // STEPS
    passes = relay_passes(outer)
    taps = r.conv_x.shape[0]
    dtype = r.x_buf.dtype

    near = seq + 1 - 2 * lax.rem(seq, 2)
    side = seq + 2 - 4 * lax.rem(lax.div(seq, 2), 2)
    cross = near + side - seq
    mates = (seq, near, side, cross)
    inners = tuple(lax.rem(mate, INNER) for mate in mates)

    def remote(source, target, send, recv, device):
        return pltpu.make_async_remote_copy(
            src_ref=source,
            dst_ref=target,
            send_sem=send,
            recv_sem=recv,
            device_id=device,
            device_id_type=MESH,
        )

    def head_of(step):
        return lax.rem(head + step, heads)

    def received(view, sem):
        remote(view, view, r.spare.at[0], sem, (near, head)).wait_recv()

    def sent(view, sem):
        remote(view, view, sem, r.spare.at[0], (near, head)).wait_send()

    barrier = pltpu.get_barrier_semaphore()
    gives_halo = jnp.logical_and(head == heads - 1, seq < count - 1)
    takes_halo = seq > 0
    gives_out = jnp.logical_and(gives_halo, inner == INNER - 1)
    takes_out = jnp.logical_and(takes_halo, inner == 0)

    def greet(where, which):
        pl.semaphore_signal(barrier, inc=1, device_id=(where, which), device_id_type=MESH)

    for index, mate in enumerate(mates):
        for step in range(heads):
            if index or step:
                greet(mate, head_of(step))
    expected = jnp.int32(INNER * heads - 1)
    for sign in (1, -1):
        for distance in (1, 2):
            there = level + sign * distance
            exists = jnp.logical_and(there >= 0, there < outer)

            @pl.when(exists)
            def _(there=there):
                greet(there * INNER + inner, head)

            expected = expected + jnp.where(exists, 1, 0)

    @pl.when(gives_out)
    def _():
        for which in range(heads):
            greet(seq + 1, which)

    @pl.when(takes_out)
    def _():
        greet(seq - 1, heads - 1)

    expected = expected + jnp.where(gives_out, heads, 0) + jnp.where(takes_out, 1, 0)
    mine = pl.ds(pl.multiple_of(head * rows, 16), rows)
    plan = (
        (r.b_in, r.b_buf, STATE),
        (r.c_in, r.c_buf, STATE),
        (r.x_in, r.x_buf, width),
        (r.z_in, r.z_buf, width),
    )
    halos = ((r.x_in, r.x_halo), (r.b_in, r.b_halo), (r.c_in, r.c_halo))

    def halo_copy(index, which, device):
        source, target = halos[index]
        size = target.shape[1]
        return remote(
            source.at[pl.ds(rows - HALO, HALO), pl.ds(which * size, size)],
            target,
            r.halo_send.at[index, which],
            r.halo_recv.at[index],
            device,
        )

    def entry_view(kind, which, g):
        source, target, size = plan[kind]
        low = pl.multiple_of((which * groups + g) * size, LANES)
        return source.at[:, pl.ds(low, size)], target.at[g, mine]

    def entry_copy(kind, g, step):
        source, target = entry_view(kind, head_of(step), g)
        return remote(
            source,
            target,
            r.entry_send.at[kind, step - 1],
            r.entry_recv.at[kind, step - 1, g],
            (seq, head_of(step)),
        )

    def own_copy(kind, g):
        source, target = entry_view(kind, head, g)
        return pltpu.make_async_copy(source, target, r.own_sems.at[kind, g])

    def dt_copy(step):
        return remote(
            r.dt_in,
            r.dt_buf.at[mine],
            r.dt_send.at[step],
            r.dt_recv.at[step],
            (seq, head_of(step)),
        )

    own_dt = pltpu.make_async_copy(r.dt_in, r.dt_buf.at[mine], r.misc_sems.at[0])
    own_weight = pltpu.make_async_copy(r.w_in, r.wv.at[level], r.misc_sems.at[1])

    own_weight.start()
    own_dt.start()
    for kind in range(4):
        for g in range(groups):
            own_copy(kind, g).start()
    with jax.named_scope("greeting"):
        pl.semaphore_wait(barrier, expected)

    for step in range(1, heads):
        dt_copy(step).start()

    @pl.when(gives_halo)
    def _():
        for index in range(len(halos)):
            for which in range(heads):
                halo_copy(index, which, (seq + 1, which)).start()

    def chunk_view(block, chunk):
        low = pl.multiple_of(lax.rem(chunk, per_half) * chunk_rows, 16)
        lines = pl.ds(low, chunk_rows)
        if halves == 1:
            return r.wv.at[block, lines]
        left = pl.multiple_of(lax.div(chunk, per_half) * half_cols, LANES)
        return r.wv.at[block, lines, pl.ds(left, half_cols)]

    def weight_item(sign, which, chunk, kinds):
        room = outer - 1 - level if sign > 0 else level
        behind = lax.div(level if sign > 0 else outer - 1 - level, 2)
        far = room >= 2
        hops = jnp.where(far, lax.div(which, 2), which)
        distance = jnp.where(far, 2 - lax.rem(which, 2), 1)
        exists = jnp.logical_and(room >= 1, hops <= behind)
        edge = level == 0 if sign > 0 else level == outer - 1
        if kinds is not None:
            way = "up" if sign > 0 else "down"
            chosen = jnp.bool_(False)
            if "edge " + way in kinds:
                chosen = jnp.logical_or(chosen, jnp.logical_and(far, edge))
            if "last " + way in kinds:
                chosen = jnp.logical_or(chosen, jnp.logical_not(far))
            if "mid " + way in kinds:
                chosen = jnp.logical_or(chosen, jnp.logical_and(far, jnp.logical_not(edge)))
            exists = jnp.logical_and(exists, chosen)
        block = level - sign * 2 * hops
        target = (level + sign * distance) * INNER + inner
        view = chunk_view(block, chunk)
        copy = remote(
            view,
            view,
            r.weight_send.at[0 if sign > 0 else 1, which],
            r.weight_recv.at[block, chunk],
            (target, head),
        )
        if kinds is None:

            @pl.when(exists)
            def _():
                whole = r.wv.at[level]
                remote(
                    whole,
                    whole,
                    r.weight_send.at[0 if sign > 0 else 1, which],
                    r.weight_recv.at[level, 0],
                    (target, head),
                ).wait_send()

            return
        fresh = jnp.logical_or(jnp.logical_not(far), distance == 2)
        relayed = jnp.logical_and(jnp.logical_and(exists, hops >= 1), fresh)

        @pl.when(relayed)
        def _():
            copy.wait_recv()

        @pl.when(exists)
        def _():
            copy.start()

    def weight_pass(which, kinds, low=0, high=CHUNKS):
        def body(chunk, carry):
            for sign, way in ((1, "up"), (-1, "down")):
                if any(kind.endswith(way) for kind in kinds):
                    weight_item(sign, which, chunk, kinds)
            return carry

        lax.fori_loop(low, high, body, 0)

    def weight_arrived(block, chunk):
        below = block < level
        apart = jnp.where(below, level - block, block - level)
        room = jnp.where(below, outer - 1 - level, level)
        relayed = jnp.logical_and(lax.rem(apart, 2) == 0, room >= 1)

        @pl.when(jnp.logical_and(apart > 0, jnp.logical_not(relayed)))
        def _():
            view = chunk_view(block, chunk)
            remote(
                view,
                view,
                r.weight_send.at[0, 0],
                r.weight_recv.at[block, chunk],
                (seq, head),
            ).wait_recv()

    for step in range(1, heads):
        for kind in range(3):
            entry_copy(kind, 0, step).start()
    own_weight.wait()
    if passes > 1:
        weight_pass(1, ("edge up", "edge down", "mid up"), 0, OPENING)
    if passes:
        weight_pass(0, ("edge up", "edge down", "last up", "last down", "mid down"), 0, BEFORE)
        weight_pass(0, ("edge down", "last up", "last down", "mid down"), BEFORE)

    for g in range(1, groups):
        for kind in range(3):
            for step in range(1, heads):
                entry_copy(kind, g, step).start()
    for g in range(groups):
        for step in range(1, heads):
            entry_copy(3, g, step).start()

    r.params[...] = jnp.zeros_like(r.params)
    r.params[0:1, 0:local_heads] = r.dt_bias[...]
    r.params[1:2, 0:local_heads] = r.a_log[...]
    columns = r.params[...].T
    bias = columns[0:local_heads, 0:1]
    coeff = -jnp.exp(columns[0:local_heads, 1:2])
    own_dt.wait()
    for step in range(1, heads):
        dt_copy(step).wait_recv()
    early = lax.broadcasted_iota(jnp.int32, (SPAN, SPAN), 0)
    late = lax.broadcasted_iota(jnp.int32, (SPAN, SPAN), 1)
    prefix_ones = jnp.where(early <= late, 1.0, 0.0).astype(jnp.float32)
    r.cum_pad[...] = jnp.zeros_like(r.cum_pad)
    log_total = jnp.zeros((1, LANES), jnp.float32)
    for block in range(blocks):
        span = slice(block * SPAN, (block + 1) * SPAN)
        r.dt_t[...] = r.dt_buf[span, :].astype(jnp.float32).T
        raw = r.dt_t[pl.ds(pl.multiple_of(head * local_heads, 8), local_heads), :] + bias
        step_size = jnp.maximum(raw, 0.0) + jnp.log1p(jnp.exp(-jnp.abs(raw)))
        r.step_t[:, span] = step_size
        summed = jnp.dot(
            coeff * step_size,
            prefix_ones,
            preferred_element_type=jnp.float32,
            precision=lax.Precision.HIGHEST,
        )
        r.cum_t[:, span] = summed
        r.cum_pad[0:local_heads, :] = summed
        by_token = r.cum_pad[...].T
        log_total = log_total + by_token[SPAN - 1 : SPAN, :]
        for g in range(groups):
            shift = (LANES - g * per) % LANES
            r.cum_c[g, span, :] = pltpu.roll(by_token, shift, 1) if shift else by_token
    logs = jnp.broadcast_to(log_total, (8, LANES))
    r.log_out[...] = logs
    r.log_in[inner] = logs

    def log_copy(index):
        return remote(
            r.log_out,
            r.log_in.at[inner],
            r.log_sems.at[0],
            r.log_sems.at[1],
            (mates[index], head),
        )

    for index in range(1, INNER):
        log_copy(index).start()

    @pl.when(jnp.logical_not(takes_halo))
    def _():
        for _, target in halos:
            target[...] = jnp.zeros_like(target)

    @pl.when(takes_halo)
    def _():
        for index in range(len(halos)):
            halo_copy(index, 0, (seq, head)).wait_recv()

    @pl.when(level == 0)
    def _():
        r.chain_in[...] = jnp.zeros_like(r.chain_in)

    causal = early >= late

    def piece_copy(g, index):
        low = pl.multiple_of(inners[index] * part, 16)
        return remote(
            r.final_out.at[g, pl.ds(low, part)],
            r.piece_in.at[g, inner],
            r.piece_send.at[0],
            r.piece_recv.at[g],
            (mates[index], head),
        )

    def local(g, carry):
        with jax.named_scope("local_wait"):
            for kind in range(3):
                own_copy(kind, g).wait()
                for step in range(1, heads):
                    entry_copy(kind, g, step).wait_recv()
        wide = pl.ds(pl.multiple_of(g * width, LANES), width)
        slim = pl.ds(pl.multiple_of(g * STATE, LANES), STATE)
        x_conv = conv_silu(
            r.x_buf[g],
            r.x_halo[HALO - 8 : HALO, wide],
            [r.conv_x[tap : tap + 1, wide] for tap in range(taps)],
            r.bias_x[:, wide],
            r.x_pad,
            dtype,
        )
        b_conv = conv_silu(
            r.b_buf[g],
            r.b_halo[HALO - 8 : HALO, slim],
            [r.conv_bc[tap, 0:1, slim] for tap in range(taps)],
            r.bias_bc[0:1, slim],
            r.bc_pad,
            dtype,
        )
        c_conv = conv_silu(
            r.c_buf[g],
            r.c_halo[HALO - 8 : HALO, slim],
            [r.conv_bc[tap, 1:2, slim] for tap in range(taps)],
            r.bias_bc[1:2, slim],
            r.bc_pad,
            dtype,
        )
        r.c_conv[g] = c_conv
        own_heads = pl.ds(pl.multiple_of(g * per, 8), per)
        for block in range(blocks):
            low = block * SPAN
            b_blk = b_conv[low : low + SPAN]
            c_blk = c_conv[low : low + SPAN]
            r.x_t[...] = x_conv[low : low + SPAN].astype(jnp.float32).T
            scores = lax.dot_general(c_blk, b_blk, NT, preferred_element_type=jnp.float32)
            cum_rows = r.cum_t[own_heads, low : low + SPAN]
            step_all = r.step_t[own_heads, low : low + SPAN]
            for index in range(per):
                lines = pl.ds(index * HEAD_DIM, HEAD_DIM)
                column = r.cum_c[g, low : low + SPAN, index : index + 1]
                row = cum_rows[index : index + 1, :]
                step = step_all[index : index + 1, :]
                total = row[:, SPAN - 1 : SPAN]
                decays = jnp.exp(jnp.where(causal, column - row, -jnp.inf))
                mix = (decays * step * scores).astype(dtype)
                x_head = r.x_t[lines, :]
                product = lax.dot_general(
                    x_head.astype(dtype), mix, NT, preferred_element_type=jnp.float32
                )
                r.y_t[g, block, lines, :] = product + r.skip[g * per + index] * x_head
                r.x_w[lines, :] = (x_head * (step * jnp.exp(total - row))).astype(dtype)
            piece = jnp.dot(r.x_w[...], b_blk, preferred_element_type=jnp.float32)
            if block < blocks - 1:
                r.pieces[g, block] = piece
            if block == 0:
                r.final[...] = piece
            else:
                r.running[...] = piece
                for index in range(per):
                    lines = pl.ds(index * HEAD_DIM, HEAD_DIM)
                    decay = jnp.exp(cum_rows[index : index + 1, SPAN - 1 : SPAN])
                    r.final[lines, :] = decay * r.final[lines, :] + r.running[lines, :]
        r.final_out[g] = r.final[...].astype(dtype)
        for index in range(1, INNER):
            piece_copy(g, index).start()
        own_part = pl.ds(pl.multiple_of(inner * part, 16), part)
        r.piece_in[g, inner] = r.final_out[g, own_part, :]
        return carry

    with jax.named_scope("local_all"):
        lax.fori_loop(0, groups, local, 0)
    if passes > 1:
        weight_pass(1, ("last down",), 0, RELAYED)

    def chain_copy(g, where):
        return remote(
            r.chain_out.at[g],
            r.chain_in.at[g],
            r.chain_send.at[0],
            r.chain_recv.at[g],
            (where, head),
        )

    def start_copy(g, index):
        low = pl.multiple_of(inner * part, 16)
        return remote(
            r.start_out.at[g, inners[index]],
            r.start_in.at[g, pl.ds(low, part)],
            r.start_send.at[0],
            r.start_recv.at[g],
            (mates[index], head),
        )

    received(r.log_in.at[1:INNER], r.log_sems.at[1])

    def carry_step(g, carry):
        with jax.named_scope("carry_wait"):
            received(r.piece_in.at[g, 1:INNER], r.piece_recv.at[g])

            @pl.when(level > 0)
            def _():
                chain_copy(g, seq).wait_recv()

        first = g * per + inner * part_heads
        state = [
            r.chain_in[g, index * HEAD_DIM : (index + 1) * HEAD_DIM, :].astype(jnp.float32)
            for index in range(part_heads)
        ]
        for position in range(INNER):
            decays = jnp.exp(pltpu.roll(r.log_in[position], lax.rem(LANES - first, LANES), 1))
            for index in range(part_heads):
                lines = slice(index * HEAD_DIM, (index + 1) * HEAD_DIM)
                r.start_out[g, position, lines, :] = state[index].astype(dtype)
                piece = r.piece_in[g, position, lines, :].astype(jnp.float32)
                state[index] = decays[0:1, index : index + 1] * state[index] + piece
        for index in range(part_heads):
            r.chain_out[g, index * HEAD_DIM : (index + 1) * HEAD_DIM, :] = state[index].astype(
                dtype
            )

        @pl.when(level < outer - 1)
        def _():
            chain_copy(g, seq + INNER).start()

        for index in range(1, INNER):
            start_copy(g, index).start()
        own_part = pl.ds(pl.multiple_of(inner * part, 16), part)
        r.start_in[g, own_part, :] = r.start_out[g, inner]
        return carry

    with jax.named_scope("carry_all"):
        lax.fori_loop(0, groups, carry_step, 0)

    with jax.named_scope("chain_left"):

        @pl.when(level < outer - 1)
        def _():
            sent(r.chain_out, r.chain_send.at[0])

    if passes > 1:
        with jax.named_scope("pass_one_early"):
            weight_pass(1, ("edge up", "mid up"), OPENING, OPENING + FIRST)
            weight_pass(1, ("edge down",), OPENING)
            weight_pass(1, ("last down",), RELAYED)
            weight_pass(1, ("mid down",))
            weight_pass(1, ("last up",), 0, BEFORE)

    def share_copy(g, index):
        target = r.a_buf.at[g, pl.ds(index * tokens, tokens)]
        return remote(
            r.a_buf.at[g, pl.ds(0, tokens)],
            target,
            r.share_send.at[0],
            r.share_recv.at[g] if index == 2 else r.near_recv.at[0],
            (mates[index], head),
        )

    def forward_copy(g):
        return remote(
            r.a_buf.at[g, pl.ds(2 * tokens, tokens)],
            r.a_buf.at[g, pl.ds(3 * tokens, tokens)],
            r.share_send.at[0],
            r.near_recv.at[1],
            (near, head),
        )

    def norm_step(g, carry):
        with jax.named_scope("norm_wait"):
            received(r.start_in.at[g, pl.ds(0, (INNER - 1) * part)], r.start_recv.at[g])
            own_copy(3, g).wait()
            for step in range(1, heads):
                entry_copy(3, g, step).wait_recv()
        wide = pl.ds(pl.multiple_of(g * width, LANES), width)
        own_heads = pl.ds(pl.multiple_of(g * per, 8), per)
        r.running[...] = r.start_in[g].astype(jnp.float32)
        for block in range(blocks):
            low = block * SPAN
            c_blk = r.c_conv[g, low : low + SPAN, :]
            r.x_t[...] = lax.dot_general(
                r.running[...].astype(dtype), c_blk, NT, preferred_element_type=jnp.float32
            )
            grown = jnp.exp(r.cum_t[own_heads, low : low + SPAN])
            for index in range(per):
                lines = pl.ds(index * HEAD_DIM, HEAD_DIM)
                row = grown[index : index + 1, :]
                r.x_t[lines, :] = r.y_t[g, block, lines, :] + r.x_t[lines, :] * row
                if block < blocks - 1:
                    r.running[lines, :] = (
                        row[:, SPAN - 1 : SPAN] * r.running[lines, :]
                        + r.pieces[g, block, lines, :]
                    )
            gate = r.z_buf[g, low : low + SPAN, :].astype(jnp.float32)
            gated = r.x_t[...].T * (gate / (1.0 + jnp.exp(-gate)))
            mean = jnp.sum(gated * gated, axis=-1, keepdims=True) * (1.0 / width)
            normed = gated * lax.rsqrt(mean + 1.0)
            r.a_buf[g, low : low + SPAN, :] = (normed * r.gain[:, wide]).astype(dtype)
        share_copy(g, 2).start()
        share_copy(g, 1).start()

        if passes:

            @pl.when(g == min(LATE_GROUP, groups - 1))
            def _():
                weight_pass(0, ("edge up",), BEFORE)
                weight_pass(0, ("mid up",))

        return carry

    with jax.named_scope("norm_all"):
        lax.fori_loop(0, groups, norm_step, 0)

    if passes > 1:
        with jax.named_scope("pass_one_late"):
            weight_pass(1, ("edge up", "mid up"), OPENING + FIRST)
            weight_pass(1, ("last up",), BEFORE)

    def later_pass(which, carry):
        for part in ("edge", "last", "mid"):
            weight_pass(which, (part + " up", part + " down"))
        return carry

    if passes > 2:
        lax.fori_loop(2, passes, later_pass, 0)

    edge_order, inner_order = column_orders(outer)
    early_count = min(2, outer)
    at_edge = jnp.logical_or(level == 0, level == outer - 1)
    direction = jnp.where(level < (outer + 1) // 2, 1, -1)

    def block_at(index):
        offset = jnp.where(at_edge, edge_order[index], inner_order[index])
        return lax.rem(level + direction * offset + outer, outer)

    steps_per_group = width // step_rows

    def product(block, step, low, size, cols):
        g = lax.div(step, steps_per_group)
        off = pl.multiple_of(lax.rem(step, steps_per_group) * step_rows, LANES)
        down = pl.multiple_of(step * step_rows, 16)
        return jnp.dot(
            r.a_buf[g, low : low + size, pl.ds(off, step_rows)],
            r.wv[block, pl.ds(down, step_rows), cols],
            preferred_element_type=jnp.float32,
        )

    per_step = per_half // STEPS
    every = slice(0, tile)

    def arrive(block, step, parts):
        for which in parts:
            for extra in range(per_step):
                weight_arrived(block, which * per_half + step * per_step + extra)

    def result_copy(index, mate, which, cols, slot):
        low = pl.multiple_of(mate * tokens + which * rows, 16)
        spread = pl.ds(cols.start, cols.stop - cols.start)
        position = block_at(index) * INNER + inner
        return remote(
            r.terms.at[index, pl.ds(low, rows), spread],
            r.landed.at[head, position, :, spread],
            r.term_send.at[index, slot],
            r.term_recv.at[index, slot],
            (mates[mate], which),
        )

    def ship(index, low_mate, mate_count, cols=every, slot=0):
        for mate in range(low_mate, low_mate + mate_count):
            for which in range(heads):
                if mate == 0:

                    @pl.when(head != which)
                    def _(mate=mate, which=which):
                        result_copy(index, mate, which, cols, slot).start()

                else:
                    result_copy(index, mate, which, cols, slot).start()
        if low_mate == 0:
            own_rows = pl.ds(pl.multiple_of(head * rows, 16), rows)
            position = block_at(index) * INNER + inner
            r.landed[head, position, :, cols] = r.terms[index, own_rows, cols]

    half = 2 * tokens

    def unit(index, low, size, waits, cols=every, parts=tuple(range(halves))):
        block = block_at(index)
        r.acc[0:size, cols] = jnp.zeros((size, cols.stop - cols.start), jnp.float32)

        def body(step, carry):
            if waits:
                arrive(block, step, parts)
            r.acc[0:size, cols] += product(block, step, low, size, cols)
            return carry

        lax.fori_loop(0, STEPS, body, 0)
        r.terms[index, low : low + size, cols] = r.acc[0:size, cols].astype(dtype)

    received(r.a_buf.at[:, pl.ds(tokens, tokens)], r.near_recv.at[0])
    for index in range(early_count):
        with jax.named_scope("early_zero"):
            unit(index, 0, half, True)
            ship(index, 0, 2)

    def pass_on(g, carry):
        share_copy(g, 2).wait_recv()
        forward_copy(g).start()
        return carry

    with jax.named_scope("pass_on"):
        lax.fori_loop(0, groups, pass_on, 0)

    with jax.named_scope("passed"):
        received(r.a_buf.at[:, pl.ds(3 * tokens, tokens)], r.near_recv.at[1])
    for index in range(early_count):
        with jax.named_scope("early_one"):
            unit(index, half, half, False)
            ship(index, 2, 2)

    @pl.when(gives_halo)
    def _():
        for index in range(len(halos)):
            for which in range(heads):
                halo_copy(index, which, (seq + 1, which)).wait_send()

    for step in range(1, heads):
        dt_copy(step).wait_send()
    sent(r.log_in.at[1:INNER], r.log_sems.at[0])

    for kind, buffer in enumerate((r.b_buf, r.c_buf, r.x_buf, r.z_buf)):
        for step in range(1, heads):
            sent(buffer.at[:, mine], r.entry_send.at[kind, step - 1])
    sent(r.piece_in.at[:, 1:INNER], r.piece_send.at[0])
    sent(r.start_out.at[:, 1:INNER], r.start_send.at[0])
    sent(r.a_buf.at[:, pl.ds(0, 3 * tokens)], r.share_send.at[0])

    def parts_of(index):
        if index < outer - 1 or index < early_count:
            return [every]
        return [slice(which * half_cols, (which + 1) * half_cols) for which in range(halves)]

    def terms_view(index, cols):
        lines = pl.ds(0, (INNER * heads - 1) * rows)
        return r.terms.at[index, lines, pl.ds(cols.start, cols.stop - cols.start)]

    def results_of(index, slot, cols):
        received(terms_view(index, cols), r.term_recv.at[index, slot])

    for index in range(early_count, outer):
        parts = parts_of(index)
        for slot, cols in enumerate(parts):
            with jax.named_scope("late"):
                which = tuple(range(halves)) if len(parts) == 1 else (slot,)
                unit(index, 0, 2 * half, True, cols, which)
                ship(index, 2, 2, cols, slot)
                ship(index, 0, 2, cols, slot)

    spread = INNER * tile

    def result_out(block):
        where = pl.ds(block * spread, spread)
        return pltpu.make_async_copy(r.stage.at[:, where], r.out.at[:, where], r.misc_sems.at[2])

    def assemble(block):
        for position in range(block * INNER, (block + 1) * INNER):
            total = r.landed[0, position].astype(jnp.float32)
            for which in range(1, heads):
                total = total + r.landed[which, position].astype(jnp.float32)
            r.stage[:, position * tile : (position + 1) * tile] = total.astype(dtype)
        result_out(block).start()

    last_block = block_at(outer - 1)
    with jax.named_scope("result_wait"):
        for index in range(outer - 1):
            results_of(index, 0, every)
    with jax.named_scope("assembly"):
        for block in range(outer):
            pl.when(block != last_block)(functools.partial(assemble, block))
    with jax.named_scope("result_wait_last"):
        for slot, cols in enumerate(parts_of(outer - 1)):
            results_of(outer - 1, slot, cols)
    with jax.named_scope("assembly_last"):
        for block in range(outer):
            pl.when(block == last_block)(functools.partial(assemble, block))

    with jax.named_scope("drain"):
        pltpu.make_async_copy(r.stage, r.out, r.misc_sems.at[2]).wait()
        if passes:

            def drain_weight(which, carry):
                weight_item(1, which, 0, None)
                weight_item(-1, which, 0, None)
                return carry

            lax.fori_loop(0, passes, drain_weight, 0)
        for index in range(outer):
            for slot, cols in enumerate(parts_of(index)):
                sent(terms_view(index, cols), r.term_send.at[index, slot])


def per_device(
    x_proj,
    z_proj,
    b_proj,
    c_proj,
    dt_raw,
    dt_bias,
    a_log,
    d_skip,
    conv_x,
    conv_bias_x,
    conv_bc,
    conv_bias_bc,
    norm_weight,
    out_weight,
):
    count = lax.axis_size("seq")
    heads = lax.axis_size("head")
    outer = count // INNER
    rows = x_proj.shape[0]
    tokens = rows * heads
    cols = x_proj.shape[1] // heads
    groups = b_proj.shape[1] // heads // STATE
    width = cols // groups
    local_heads = dt_bias.shape[0]
    blocks = tokens // SPAN
    part = width // INNER
    depth, tile = out_weight.shape
    passes = max(relay_passes(outer), 1)
    dtype = x_proj.dtype
    f32 = jnp.float32
    vmem = pl.BlockSpec(memory_space=pltpu.VMEM)
    smem = pl.BlockSpec(memory_space=pltpu.SMEM)
    hbm = pl.BlockSpec(memory_space=pl.ANY)
    dma = pltpu.SemaphoreType.DMA
    inputs = {
        "x_in": (x_proj, hbm),
        "z_in": (z_proj, hbm),
        "b_in": (b_proj, hbm),
        "c_in": (c_proj, hbm),
        "dt_in": (dt_raw, hbm),
        "w_in": (out_weight, hbm),
        "dt_bias": (dt_bias[None], vmem),
        "a_log": (a_log[None], vmem),
        "skip": (d_skip, smem),
        "conv_x": (conv_x, vmem),
        "bias_x": (conv_bias_x[None], vmem),
        "conv_bc": (conv_bc, vmem),
        "bias_bc": (conv_bias_bc, vmem),
        "gain": (norm_weight[None], vmem),
    }
    scratch = {
        "x_buf": pltpu.VMEM((groups, tokens, width), dtype),
        "z_buf": pltpu.VMEM((groups, tokens, width), dtype),
        "b_buf": pltpu.VMEM((groups, tokens, STATE), dtype),
        "c_buf": pltpu.VMEM((groups, tokens, STATE), dtype),
        "dt_buf": pltpu.VMEM((tokens, dt_raw.shape[1]), dtype),
        "x_halo": pltpu.VMEM((HALO, cols), dtype),
        "b_halo": pltpu.VMEM((HALO, groups * STATE), dtype),
        "c_halo": pltpu.VMEM((HALO, groups * STATE), dtype),
        "wv": pltpu.VMEM((outer, depth, tile), dtype),
        "params": pltpu.VMEM((LANES, LANES), f32),
        "dt_t": pltpu.VMEM((dt_raw.shape[1], SPAN), f32),
        "step_t": pltpu.VMEM((local_heads, tokens), f32),
        "cum_t": pltpu.VMEM((local_heads, tokens), f32),
        "cum_pad": pltpu.VMEM((LANES, SPAN), f32),
        "cum_c": pltpu.VMEM((groups, tokens, LANES), f32),
        "log_out": pltpu.VMEM((8, LANES), f32),
        "log_in": pltpu.VMEM((INNER, 8, LANES), f32),
        "x_pad": pltpu.VMEM((tokens + 8, width), f32),
        "bc_pad": pltpu.VMEM((tokens + 8, STATE), f32),
        "x_t": pltpu.VMEM((width, SPAN), f32),
        "x_w": pltpu.VMEM((width, SPAN), dtype),
        "c_conv": pltpu.VMEM((groups, tokens, STATE), dtype),
        "y_t": pltpu.VMEM((groups, blocks, width, SPAN), f32),
        "pieces": pltpu.VMEM((groups, max(blocks - 1, 1), width, STATE), f32),
        "final": pltpu.VMEM((width, STATE), f32),
        "running": pltpu.VMEM((width, STATE), f32),
        "final_out": pltpu.VMEM((groups, width, STATE), dtype),
        "piece_in": pltpu.VMEM((groups, INNER, part, STATE), dtype),
        "chain_in": pltpu.VMEM((groups, part, STATE), dtype),
        "chain_out": pltpu.VMEM((groups, part, STATE), dtype),
        "start_out": pltpu.VMEM((groups, INNER, part, STATE), dtype),
        "start_in": pltpu.VMEM((groups, width, STATE), dtype),
        "a_buf": pltpu.VMEM((groups, INNER * tokens, width), dtype),
        "acc": pltpu.VMEM((INNER * tokens, tile), f32),
        "terms": pltpu.VMEM((outer, INNER * tokens, tile), dtype),
        "landed": pltpu.VMEM((heads, count, rows, tile), dtype),
        "entry_send": dma((4, max(heads - 1, 1))),
        "entry_recv": dma((4, max(heads - 1, 1), groups)),
        "own_sems": dma((4, groups)),
        "stage": pltpu.VMEM((rows, count * tile), dtype),
        "misc_sems": dma((3,)),
        "spare": dma((1,)),
        "dt_send": dma((heads,)),
        "dt_recv": dma((heads,)),
        "halo_send": dma((3, heads)),
        "halo_recv": dma((3,)),
        "weight_send": dma((2, passes)),
        "weight_recv": dma((outer, CHUNKS)),
        "log_sems": dma((2,)),
        "piece_send": dma((1,)),
        "piece_recv": dma((groups,)),
        "chain_send": dma((1,)),
        "chain_recv": dma((groups,)),
        "start_send": dma((1,)),
        "start_recv": dma((groups,)),
        "share_send": dma((1,)),
        "share_recv": dma((groups,)),
        "near_recv": dma((2,)),
        "term_send": dma((outer, column_halves(tile))),
        "term_recv": dma((outer, column_halves(tile))),
    }
    names = list(inputs) + ["out"] + list(scratch)
    return pl.pallas_call(
        functools.partial(mixer_kernel, count, heads, names),
        out_shape=jax.ShapeDtypeStruct((rows, count * tile), dtype),
        in_specs=[spec for _, spec in inputs.values()],
        out_specs=hbm,
        scratch_shapes=list(scratch.values()),
        compiler_params=pltpu.CompilerParams(
            collective_id=0, has_side_effects=True, vmem_limit_bytes=60 * 1024 * 1024
        ),
        name="mixer",
    )(*[value for value, _ in inputs.values()])


def solution(mesh):
    in_specs = (
        P(("seq", "head"), None),
        P(("seq", "head"), None),
        P(("seq", "head"), None),
        P(("seq", "head"), None),
        P(("seq", "head"), None),
        P("head"),
        P("head"),
        P("head"),
        P(None, "head"),
        P("head"),
        P(None, None, "head"),
        P(None, "head"),
        P("head"),
        P("head", "seq"),
    )
    out_specs = P(("seq", "head"), None)
    return jax.shard_map(
        per_device, mesh=mesh, in_specs=in_specs, out_specs=out_specs, check_vma=False
    )
```

```python
import functools
import types

import jax
import jax.numpy as jnp
from jax import lax
from jax.experimental import pallas as pl
from jax.experimental.pallas import tpu as pltpu
from jax.sharding import PartitionSpec as P

HEAD_DIM = 64
STATE = 128
SPAN = 128
HALO = 8
INNER = 4
CHUNKS = 16
STEPS = 8
OPENING = 2
BEFORE = 12
RELAYED = 4
FIRST = 4
LATE_GROUP = 3
LANES = 128
NT = (((1,), (1,)), ((), ()))
MESH = pl.DeviceIdType.MESH


def relay_passes(outer):
    passes = 0
    for level in range(outer):
        room = outer - 1 - level
        behind = level // 2 + 1
        if room >= 1:
            passes = max(passes, behind * min(room, 2))
    return max(passes, outer - 1)


def column_halves(tile):
    return 2 if tile % (2 * LANES) == 0 else 1


def column_orders(outer):
    edge = list(range(outer))
    if outer < 4:
        return edge, edge, edge
    first = [0, 2, outer - 1, 1]
    top = [0, 1] + list(range(outer - 1, 1, -1))
    return edge, first + [offset for offset in edge if offset not in first], top


def conv_silu(value, halo, taps_of, bias, padded, dtype):
    tokens = value.shape[0]
    padded[0:8, :] = halo.astype(jnp.float32)
    padded[8 : 8 + tokens, :] = value.astype(jnp.float32)
    total = bias + jnp.zeros(value.shape, jnp.float32)
    taps = len(taps_of)
    for offset in range(taps):
        low = 8 - (taps - 1) + offset
        total = total + taps_of[offset] * padded[low : low + tokens, :]
    return (total / (1.0 + jnp.exp(-total))).astype(dtype)


def mixer_kernel(count, heads, names, *refs):
    r = types.SimpleNamespace(**dict(zip(names, refs)))
    seq = lax.axis_index("seq")
    head = lax.axis_index("head")
    outer = count // INNER
    inner = lax.rem(seq, INNER)
    level = lax.div(seq, INNER)
    rows = r.x_in.shape[0]
    tokens = rows * heads
    groups, _, width = r.x_buf.shape
    per = width // HEAD_DIM
    blocks = tokens // SPAN
    local_heads = groups * per
    part = width // INNER
    part_heads = part // HEAD_DIM
    depth = r.wv.shape[1]
    tile = r.wv.shape[2]
    halves = column_halves(tile)
    half_cols = tile // halves
    per_half = CHUNKS // halves
    chunk_rows = depth // per_half
    step_rows = depth // STEPS
    passes = relay_passes(outer)
    taps = r.conv_x.shape[0]
    dtype = r.x_buf.dtype

    near = seq + 1 - 2 * lax.rem(seq, 2)
    side = seq + 2 - 4 * lax.rem(lax.div(seq, 2), 2)
    cross = near + side - seq
    mates = (seq, near, side, cross)
    inners = tuple(lax.rem(mate, INNER) for mate in mates)

    def remote(source, target, send, recv, device):
        return pltpu.make_async_remote_copy(
            src_ref=source,
            dst_ref=target,
            send_sem=send,
            recv_sem=recv,
            device_id=device,
            device_id_type=MESH,
        )

    def head_of(step):
        return lax.rem(head + step, heads)

    def received(view, sem):
        remote(view, view, r.spare.at[0], sem, (near, head)).wait_recv()

    def sent(view, sem):
        remote(view, view, sem, r.spare.at[0], (near, head)).wait_send()

    barrier = pltpu.get_barrier_semaphore()
    gives_halo = jnp.logical_and(head == heads - 1, seq < count - 1)
    takes_halo = seq > 0
    gives_out = jnp.logical_and(gives_halo, inner == INNER - 1)
    takes_out = jnp.logical_and(takes_halo, inner == 0)

    def greet(where, which):
        pl.semaphore_signal(barrier, inc=1, device_id=(where, which), device_id_type=MESH)

    for index, mate in enumerate(mates):
        for step in range(heads):
            if index or step:
                greet(mate, head_of(step))
    expected = jnp.int32(INNER * heads - 1)
    for sign in (1, -1):
        for distance in (1, 2):
            there = level + sign * distance
            exists = jnp.logical_and(there >= 0, there < outer)

            @pl.when(exists)
            def _(there=there):
                greet(there * INNER + inner, head)

            expected = expected + jnp.where(exists, 1, 0)

    @pl.when(gives_out)
    def _():
        for which in range(heads):
            greet(seq + 1, which)

    @pl.when(takes_out)
    def _():
        greet(seq - 1, heads - 1)

    expected = expected + jnp.where(gives_out, heads, 0) + jnp.where(takes_out, 1, 0)
    mine = pl.ds(pl.multiple_of(head * rows, 16), rows)
    plan = (
        (r.b_in, r.b_buf, STATE),
        (r.c_in, r.c_buf, STATE),
        (r.x_in, r.x_buf, width),
        (r.z_in, r.z_buf, width),
    )
    halos = ((r.x_in, r.x_halo), (r.b_in, r.b_halo), (r.c_in, r.c_halo))

    def halo_copy(index, which, device):
        source, target = halos[index]
        size = target.shape[1]
        return remote(
            source.at[pl.ds(rows - HALO, HALO), pl.ds(which * size, size)],
            target,
            r.halo_send.at[index, which],
            r.halo_recv.at[index],
            device,
        )

    def entry_view(kind, which, g):
        source, target, size = plan[kind]
        low = pl.multiple_of((which * groups + g) * size, LANES)
        return source.at[:, pl.ds(low, size)], target.at[g, mine]

    def entry_copy(kind, g, step):
        source, target = entry_view(kind, head_of(step), g)
        return remote(
            source,
            target,
            r.entry_send.at[kind, step - 1],
            r.entry_recv.at[kind, step - 1, g],
            (seq, head_of(step)),
        )

    def own_copy(kind, g):
        source, target = entry_view(kind, head, g)
        return pltpu.make_async_copy(source, target, r.own_sems.at[kind, g])

    def dt_copy(step):
        return remote(
            r.dt_in,
            r.dt_buf.at[mine],
            r.dt_send.at[step],
            r.dt_recv.at[step],
            (seq, head_of(step)),
        )

    own_dt = pltpu.make_async_copy(r.dt_in, r.dt_buf.at[mine], r.misc_sems.at[0])
    own_weight = pltpu.make_async_copy(r.w_in, r.wv.at[level], r.misc_sems.at[1])

    own_weight.start()
    own_dt.start()
    for kind in range(4):
        for g in range(groups):
            own_copy(kind, g).start()
    with jax.named_scope("greeting"):
        pl.semaphore_wait(barrier, expected)

    for step in range(1, heads):
        dt_copy(step).start()

    @pl.when(gives_halo)
    def _():
        for index in range(len(halos)):
            for which in range(heads):
                halo_copy(index, which, (seq + 1, which)).start()

    def chunk_view(block, chunk):
        low = pl.multiple_of(lax.rem(chunk, per_half) * chunk_rows, 16)
        lines = pl.ds(low, chunk_rows)
        if halves == 1:
            return r.wv.at[block, lines]
        left = pl.multiple_of(lax.div(chunk, per_half) * half_cols, LANES)
        return r.wv.at[block, lines, pl.ds(left, half_cols)]

    def down_item(which):
        sign = -1
        room = level
        behind = lax.div(outer - 1 - level, 2)
        far = room >= 2
        hops = jnp.where(far, lax.div(which, 2), which)
        distance = jnp.where(far, 2 - lax.rem(which, 2), 1)
        exists = jnp.logical_and(room >= 1, hops <= behind)
        edge = level == outer - 1
        block = level - sign * 2 * hops
        target = (level + sign * distance) * INNER + inner
        fresh = jnp.logical_or(jnp.logical_not(far), distance == 2)
        waits = jnp.logical_and(hops >= 1, fresh)
        return exists, block, target, waits, far, edge

    def up_item(which):
        room = outer - 1 - level
        own = which == 0
        skips = jnp.logical_and(own, room >= 2)
        bottom = jnp.where(skips, 2, 1)
        first = jnp.logical_or(jnp.logical_and(own, room >= 2), which == 1)
        some = jnp.logical_or(own, jnp.logical_and(level >= 2, which <= level))
        exists = jnp.logical_and(room >= 1, jnp.where(level == 0, first, some))
        block = jnp.where(level == 0, 0, jnp.where(own, level, which - 1))
        target = (level + jnp.where(level == 0, bottom, 1)) * INNER + inner
        waits = jnp.logical_and(level > 0, jnp.logical_not(own))
        return exists, block, target, waits, room >= 2, level == 0

    def weight_item(sign, which, chunk, kinds):
        item = up_item(which) if sign > 0 else down_item(which)
        exists, block, target, waits, far, edge = item
        if kinds is not None:
            way = "up" if sign > 0 else "down"
            chosen = jnp.bool_(False)
            if "edge " + way in kinds:
                chosen = jnp.logical_or(chosen, jnp.logical_and(far, edge))
            if "last " + way in kinds:
                chosen = jnp.logical_or(chosen, jnp.logical_not(far))
            if "mid " + way in kinds:
                chosen = jnp.logical_or(chosen, jnp.logical_and(far, jnp.logical_not(edge)))
            exists = jnp.logical_and(exists, chosen)
        view = chunk_view(block, chunk)
        copy = remote(
            view,
            view,
            r.weight_send.at[0 if sign > 0 else 1, which],
            r.weight_recv.at[block, chunk],
            (target, head),
        )
        if kinds is None:

            @pl.when(exists)
            def _():
                whole = r.wv.at[level]
                remote(
                    whole,
                    whole,
                    r.weight_send.at[0 if sign > 0 else 1, which],
                    r.weight_recv.at[level, 0],
                    (target, head),
                ).wait_send()

            return

        @pl.when(jnp.logical_and(exists, waits))
        def _():
            copy.wait_recv()

        @pl.when(exists)
        def _():
            copy.start()

    def weight_pass(which, kinds, low=0, high=CHUNKS):
        def body(chunk, carry):
            for sign, way in ((1, "up"), (-1, "down")):
                if any(kind.endswith(way) for kind in kinds):
                    weight_item(sign, which, chunk, kinds)
            return carry

        lax.fori_loop(low, high, body, 0)

    def weight_arrived(block, chunk):
        below = block < level
        apart = jnp.where(below, level - block, block - level)
        from_below = jnp.logical_and(level >= 2, level < outer - 1)
        from_above = jnp.logical_and(lax.rem(apart, 2) == 0, level >= 1)
        relayed = jnp.where(below, from_below, from_above)

        @pl.when(jnp.logical_and(apart > 0, jnp.logical_not(relayed)))
        def _():
            view = chunk_view(block, chunk)
            remote(
                view,
                view,
                r.weight_send.at[0, 0],
                r.weight_recv.at[block, chunk],
                (seq, head),
            ).wait_recv()

    for step in range(1, heads):
        for kind in range(3):
            entry_copy(kind, 0, step).start()
    own_weight.wait()
    if passes > 1:
        weight_pass(1, ("edge up", "edge down"), 0, OPENING)
        weight_pass(0, ("mid up",), 0, OPENING)
    if passes:
        weight_pass(0, ("edge up", "edge down", "last up", "last down", "mid down"), 0, BEFORE)
        weight_pass(0, ("edge down", "last up", "last down", "mid down"), BEFORE)

    for g in range(1, groups):
        for kind in range(3):
            for step in range(1, heads):
                entry_copy(kind, g, step).start()
    for g in range(groups):
        for step in range(1, heads):
            entry_copy(3, g, step).start()

    r.params[...] = jnp.zeros_like(r.params)
    r.params[0:1, 0:local_heads] = r.dt_bias[...]
    r.params[1:2, 0:local_heads] = r.a_log[...]
    columns = r.params[...].T
    bias = columns[0:local_heads, 0:1]
    coeff = -jnp.exp(columns[0:local_heads, 1:2])
    own_dt.wait()
    for step in range(1, heads):
        dt_copy(step).wait_recv()
    early = lax.broadcasted_iota(jnp.int32, (SPAN, SPAN), 0)
    late = lax.broadcasted_iota(jnp.int32, (SPAN, SPAN), 1)
    prefix_ones = jnp.where(early <= late, 1.0, 0.0).astype(jnp.float32)
    r.cum_pad[...] = jnp.zeros_like(r.cum_pad)
    log_total = jnp.zeros((1, LANES), jnp.float32)
    for block in range(blocks):
        span = slice(block * SPAN, (block + 1) * SPAN)
        r.dt_t[...] = r.dt_buf[span, :].astype(jnp.float32).T
        raw = r.dt_t[pl.ds(pl.multiple_of(head * local_heads, 8), local_heads), :] + bias
        step_size = jnp.maximum(raw, 0.0) + jnp.log1p(jnp.exp(-jnp.abs(raw)))
        r.step_t[:, span] = step_size
        summed = jnp.dot(
            coeff * step_size,
            prefix_ones,
            preferred_element_type=jnp.float32,
            precision=lax.Precision.HIGHEST,
        )
        r.cum_t[:, span] = summed
        r.cum_pad[0:local_heads, :] = summed
        by_token = r.cum_pad[...].T
        log_total = log_total + by_token[SPAN - 1 : SPAN, :]
        for g in range(groups):
            shift = (LANES - g * per) % LANES
            r.cum_c[g, span, :] = pltpu.roll(by_token, shift, 1) if shift else by_token
    logs = jnp.broadcast_to(log_total, (8, LANES))
    r.log_out[...] = logs
    r.log_in[inner] = logs

    def log_copy(index):
        return remote(
            r.log_out,
            r.log_in.at[inner],
            r.log_sems.at[0],
            r.log_sems.at[1],
            (mates[index], head),
        )

    for index in range(1, INNER):
        log_copy(index).start()

    @pl.when(jnp.logical_not(takes_halo))
    def _():
        for _, target in halos:
            target[...] = jnp.zeros_like(target)

    @pl.when(takes_halo)
    def _():
        for index in range(len(halos)):
            halo_copy(index, 0, (seq, head)).wait_recv()

    @pl.when(level == 0)
    def _():
        r.chain_in[...] = jnp.zeros_like(r.chain_in)

    causal = early >= late

    def piece_copy(g, index):
        low = pl.multiple_of(inners[index] * part, 16)
        return remote(
            r.final_out.at[g, pl.ds(low, part)],
            r.piece_in.at[g, inner],
            r.piece_send.at[0],
            r.piece_recv.at[g],
            (mates[index], head),
        )

    def local(g, carry):
        with jax.named_scope("local_wait"):
            for kind in range(3):
                own_copy(kind, g).wait()
                for step in range(1, heads):
                    entry_copy(kind, g, step).wait_recv()
        wide = pl.ds(pl.multiple_of(g * width, LANES), width)
        slim = pl.ds(pl.multiple_of(g * STATE, LANES), STATE)
        x_conv = conv_silu(
            r.x_buf[g],
            r.x_halo[HALO - 8 : HALO, wide],
            [r.conv_x[tap : tap + 1, wide] for tap in range(taps)],
            r.bias_x[:, wide],
            r.x_pad,
            dtype,
        )
        b_conv = conv_silu(
            r.b_buf[g],
            r.b_halo[HALO - 8 : HALO, slim],
            [r.conv_bc[tap, 0:1, slim] for tap in range(taps)],
            r.bias_bc[0:1, slim],
            r.bc_pad,
            dtype,
        )
        c_conv = conv_silu(
            r.c_buf[g],
            r.c_halo[HALO - 8 : HALO, slim],
            [r.conv_bc[tap, 1:2, slim] for tap in range(taps)],
            r.bias_bc[1:2, slim],
            r.bc_pad,
            dtype,
        )
        r.c_conv[g] = c_conv
        own_heads = pl.ds(pl.multiple_of(g * per, 8), per)
        for block in range(blocks):
            low = block * SPAN
            b_blk = b_conv[low : low + SPAN]
            c_blk = c_conv[low : low + SPAN]
            r.x_t[...] = x_conv[low : low + SPAN].astype(jnp.float32).T
            scores = lax.dot_general(c_blk, b_blk, NT, preferred_element_type=jnp.float32)
            cum_rows = r.cum_t[own_heads, low : low + SPAN]
            step_all = r.step_t[own_heads, low : low + SPAN]
            for index in range(per):
                lines = pl.ds(index * HEAD_DIM, HEAD_DIM)
                column = r.cum_c[g, low : low + SPAN, index : index + 1]
                row = cum_rows[index : index + 1, :]
                step = step_all[index : index + 1, :]
                total = row[:, SPAN - 1 : SPAN]
                decays = jnp.exp(jnp.where(causal, column - row, -jnp.inf))
                mix = (decays * step * scores).astype(dtype)
                x_head = r.x_t[lines, :]
                product = lax.dot_general(
                    x_head.astype(dtype), mix, NT, preferred_element_type=jnp.float32
                )
                r.y_t[g, block, lines, :] = product + r.skip[g * per + index] * x_head
                r.x_w[lines, :] = (x_head * (step * jnp.exp(total - row))).astype(dtype)
            piece = jnp.dot(r.x_w[...], b_blk, preferred_element_type=jnp.float32)
            if block < blocks - 1:
                r.pieces[g, block] = piece
            if block == 0:
                r.final[...] = piece
            else:
                r.running[...] = piece
                for index in range(per):
                    lines = pl.ds(index * HEAD_DIM, HEAD_DIM)
                    decay = jnp.exp(cum_rows[index : index + 1, SPAN - 1 : SPAN])
                    r.final[lines, :] = decay * r.final[lines, :] + r.running[lines, :]
        r.final_out[g] = r.final[...].astype(dtype)
        for index in range(1, INNER):
            piece_copy(g, index).start()
        own_part = pl.ds(pl.multiple_of(inner * part, 16), part)
        r.piece_in[g, inner] = r.final_out[g, own_part, :]
        return carry

    with jax.named_scope("local_all"):
        lax.fori_loop(0, groups, local, 0)
    if passes > 1:
        weight_pass(1, ("last down",), 0, RELAYED)

    def chain_copy(g, where):
        return remote(
            r.chain_out.at[g],
            r.chain_in.at[g],
            r.chain_send.at[0],
            r.chain_recv.at[g],
            (where, head),
        )

    def start_copy(g, index):
        low = pl.multiple_of(inner * part, 16)
        return remote(
            r.start_out.at[g, inners[index]],
            r.start_in.at[g, pl.ds(low, part)],
            r.start_send.at[0],
            r.start_recv.at[g],
            (mates[index], head),
        )

    received(r.log_in.at[1:INNER], r.log_sems.at[1])

    def carry_step(g, carry):
        with jax.named_scope("carry_wait"):
            received(r.piece_in.at[g, 1:INNER], r.piece_recv.at[g])

            @pl.when(level > 0)
            def _():
                chain_copy(g, seq).wait_recv()

        first = g * per + inner * part_heads
        state = [
            r.chain_in[g, index * HEAD_DIM : (index + 1) * HEAD_DIM, :].astype(jnp.float32)
            for index in range(part_heads)
        ]
        for position in range(INNER):
            decays = jnp.exp(pltpu.roll(r.log_in[position], lax.rem(LANES - first, LANES), 1))
            for index in range(part_heads):
                lines = slice(index * HEAD_DIM, (index + 1) * HEAD_DIM)
                r.start_out[g, position, lines, :] = state[index].astype(dtype)
                piece = r.piece_in[g, position, lines, :].astype(jnp.float32)
                state[index] = decays[0:1, index : index + 1] * state[index] + piece
        for index in range(part_heads):
            r.chain_out[g, index * HEAD_DIM : (index + 1) * HEAD_DIM, :] = state[index].astype(
                dtype
            )

        @pl.when(level < outer - 1)
        def _():
            chain_copy(g, seq + INNER).start()

        for index in range(1, INNER):
            start_copy(g, index).start()
        own_part = pl.ds(pl.multiple_of(inner * part, 16), part)
        r.start_in[g, own_part, :] = r.start_out[g, inner]
        return carry

    with jax.named_scope("carry_all"):
        lax.fori_loop(0, groups, carry_step, 0)

    with jax.named_scope("chain_left"):

        @pl.when(level < outer - 1)
        def _():
            sent(r.chain_out, r.chain_send.at[0])

    if passes > 1:
        with jax.named_scope("pass_one_early"):
            weight_pass(1, ("edge up",), OPENING, OPENING + FIRST)
            weight_pass(0, ("mid up",), OPENING)
            weight_pass(1, ("edge down",), OPENING)
            weight_pass(1, ("last down",), RELAYED)
            weight_pass(1, ("mid down",))
            weight_pass(1, ("last up",), 0, BEFORE)

    def share_copy(g, index):
        target = r.a_buf.at[g, pl.ds(index * tokens, tokens)]
        return remote(
            r.a_buf.at[g, pl.ds(0, tokens)],
            target,
            r.share_send.at[0],
            r.share_recv.at[g] if index == 2 else r.near_recv.at[0],
            (mates[index], head),
        )

    def forward_copy(g):
        return remote(
            r.a_buf.at[g, pl.ds(2 * tokens, tokens)],
            r.a_buf.at[g, pl.ds(3 * tokens, tokens)],
            r.share_send.at[0],
            r.near_recv.at[1],
            (near, head),
        )

    def norm_step(g, carry):
        with jax.named_scope("norm_wait"):
            received(r.start_in.at[g, pl.ds(0, (INNER - 1) * part)], r.start_recv.at[g])
            own_copy(3, g).wait()
            for step in range(1, heads):
                entry_copy(3, g, step).wait_recv()
        wide = pl.ds(pl.multiple_of(g * width, LANES), width)
        own_heads = pl.ds(pl.multiple_of(g * per, 8), per)
        r.running[...] = r.start_in[g].astype(jnp.float32)
        for block in range(blocks):
            low = block * SPAN
            c_blk = r.c_conv[g, low : low + SPAN, :]
            r.x_t[...] = lax.dot_general(
                r.running[...].astype(dtype), c_blk, NT, preferred_element_type=jnp.float32
            )
            grown = jnp.exp(r.cum_t[own_heads, low : low + SPAN])
            for index in range(per):
                lines = pl.ds(index * HEAD_DIM, HEAD_DIM)
                row = grown[index : index + 1, :]
                r.x_t[lines, :] = r.y_t[g, block, lines, :] + r.x_t[lines, :] * row
                if block < blocks - 1:
                    r.running[lines, :] = (
                        row[:, SPAN - 1 : SPAN] * r.running[lines, :]
                        + r.pieces[g, block, lines, :]
                    )
            gate = r.z_buf[g, low : low + SPAN, :].astype(jnp.float32)
            gated = r.x_t[...].T * (gate / (1.0 + jnp.exp(-gate)))
            mean = jnp.sum(gated * gated, axis=-1, keepdims=True) * (1.0 / width)
            normed = gated * lax.rsqrt(mean + 1.0)
            r.a_buf[g, low : low + SPAN, :] = (normed * r.gain[:, wide]).astype(dtype)
        share_copy(g, 2).start()
        share_copy(g, 1).start()

        if passes:

            @pl.when(g == min(LATE_GROUP, groups - 1))
            def _():
                weight_pass(0, ("edge up",), BEFORE)

        return carry

    with jax.named_scope("norm_all"):
        lax.fori_loop(0, groups, norm_step, 0)

    if passes > 1:
        with jax.named_scope("pass_one_late"):
            weight_pass(1, ("edge up",), OPENING + FIRST)
            weight_pass(1, ("last up",), BEFORE)
            if outer > 4:
                weight_pass(1, ("mid up",))

    def later_pass(which, carry):
        for part in ("edge", "last", "mid"):
            weight_pass(which, (part + " up", part + " down"))
        return carry

    edge_order, inner_order, top_order = column_orders(outer)
    early_count = min(2, outer)
    direction = jnp.where(level < (outer + 1) // 2, 1, -1)

    def block_at(index):
        offset = jnp.where(level == outer - 1, top_order[index], inner_order[index])
        offset = jnp.where(level == 0, edge_order[index], offset)
        return lax.rem(level + direction * offset + outer, outer)

    steps_per_group = width // step_rows

    def product(block, step, low, size, cols):
        g = lax.div(step, steps_per_group)
        off = pl.multiple_of(lax.rem(step, steps_per_group) * step_rows, LANES)
        down = pl.multiple_of(step * step_rows, 16)
        return jnp.dot(
            r.a_buf[g, low : low + size, pl.ds(off, step_rows)],
            r.wv[block, pl.ds(down, step_rows), cols],
            preferred_element_type=jnp.float32,
        )

    per_step = per_half // STEPS
    every = slice(0, tile)

    def arrive(block, step, parts):
        for which in parts:
            for extra in range(per_step):
                weight_arrived(block, which * per_half + step * per_step + extra)

    def result_copy(index, mate, which, cols, slot):
        low = pl.multiple_of(mate * tokens + which * rows, 16)
        spread = pl.ds(cols.start, cols.stop - cols.start)
        position = block_at(index) * INNER + inner
        return remote(
            r.terms.at[index, pl.ds(low, rows), spread],
            r.landed.at[head, position, :, spread],
            r.term_send.at[index, slot],
            r.term_recv.at[index, slot],
            (mates[mate], which),
        )

    def ship(index, low_mate, mate_count, cols=every, slot=0):
        for mate in range(low_mate, low_mate + mate_count):
            for which in range(heads):
                if mate == 0:

                    @pl.when(head != which)
                    def _(mate=mate, which=which):
                        result_copy(index, mate, which, cols, slot).start()

                else:
                    result_copy(index, mate, which, cols, slot).start()
        if low_mate == 0:
            own_rows = pl.ds(pl.multiple_of(head * rows, 16), rows)
            position = block_at(index) * INNER + inner
            r.landed[head, position, :, cols] = r.terms[index, own_rows, cols]

    half = 2 * tokens

    def unit(index, low, size, waits, cols=every, parts=tuple(range(halves))):
        block = block_at(index)
        r.acc[0:size, cols] = jnp.zeros((size, cols.stop - cols.start), jnp.float32)

        def body(step, carry):
            if waits:
                arrive(block, step, parts)
            r.acc[0:size, cols] += product(block, step, low, size, cols)
            return carry

        lax.fori_loop(0, STEPS, body, 0)
        r.terms[index, low : low + size, cols] = r.acc[0:size, cols].astype(dtype)

    received(r.a_buf.at[:, pl.ds(tokens, tokens)], r.near_recv.at[0])
    for index in range(early_count):
        with jax.named_scope("early_zero"):
            unit(index, 0, half, True)
            ship(index, 0, 2)

    def pass_on(g, carry):
        share_copy(g, 2).wait_recv()
        forward_copy(g).start()
        return carry

    if passes > 2:
        with jax.named_scope("later"):
            lax.fori_loop(2, passes, later_pass, 0)

    with jax.named_scope("pass_on"):
        lax.fori_loop(0, groups, pass_on, 0)

    with jax.named_scope("passed"):
        received(r.a_buf.at[:, pl.ds(3 * tokens, tokens)], r.near_recv.at[1])
    for index in range(early_count):
        with jax.named_scope("early_one"):
            unit(index, half, half, False)
            ship(index, 2, 2)

    @pl.when(gives_halo)
    def _():
        for index in range(len(halos)):
            for which in range(heads):
                halo_copy(index, which, (seq + 1, which)).wait_send()

    for step in range(1, heads):
        dt_copy(step).wait_send()
    sent(r.log_in.at[1:INNER], r.log_sems.at[0])

    for kind, buffer in enumerate((r.b_buf, r.c_buf, r.x_buf, r.z_buf)):
        for step in range(1, heads):
            sent(buffer.at[:, mine], r.entry_send.at[kind, step - 1])
    sent(r.piece_in.at[:, 1:INNER], r.piece_send.at[0])
    sent(r.start_out.at[:, 1:INNER], r.start_send.at[0])
    sent(r.a_buf.at[:, pl.ds(0, 3 * tokens)], r.share_send.at[0])

    def parts_of(index):
        if index < outer - 1 or index < early_count:
            return [every]
        return [slice(which * half_cols, (which + 1) * half_cols) for which in range(halves)]

    def terms_view(index, cols):
        lines = pl.ds(0, (INNER * heads - 1) * rows)
        return r.terms.at[index, lines, pl.ds(cols.start, cols.stop - cols.start)]

    def results_of(index, slot, cols):
        received(terms_view(index, cols), r.term_recv.at[index, slot])

    for index in range(early_count, outer):
        parts = parts_of(index)
        for slot, cols in enumerate(parts):
            with jax.named_scope("late"):
                which = tuple(range(halves)) if len(parts) == 1 else (slot,)
                unit(index, 0, 2 * half, True, cols, which)
                ship(index, 2, 2, cols, slot)
                ship(index, 0, 2, cols, slot)

    spread = INNER * tile

    def result_out(block):
        where = pl.ds(block * spread, spread)
        return pltpu.make_async_copy(r.stage.at[:, where], r.out.at[:, where], r.misc_sems.at[2])

    def assemble(block):
        for position in range(block * INNER, (block + 1) * INNER):
            total = r.landed[0, position].astype(jnp.float32)
            for which in range(1, heads):
                total = total + r.landed[which, position].astype(jnp.float32)
            r.stage[:, position * tile : (position + 1) * tile] = total.astype(dtype)
        result_out(block).start()

    last_block = block_at(outer - 1)
    with jax.named_scope("result_wait"):
        for index in range(outer - 1):
            results_of(index, 0, every)
    with jax.named_scope("assembly"):
        for block in range(outer):
            pl.when(block != last_block)(functools.partial(assemble, block))
    with jax.named_scope("result_wait_last"):
        for slot, cols in enumerate(parts_of(outer - 1)):
            results_of(outer - 1, slot, cols)
    with jax.named_scope("assembly_last"):
        for block in range(outer):
            pl.when(block == last_block)(functools.partial(assemble, block))

    with jax.named_scope("drain"):
        pltpu.make_async_copy(r.stage, r.out, r.misc_sems.at[2]).wait()
        if passes:

            def drain_weight(which, carry):
                weight_item(1, which, 0, None)
                weight_item(-1, which, 0, None)
                return carry

            lax.fori_loop(0, passes, drain_weight, 0)
        for index in range(outer):
            for slot, cols in enumerate(parts_of(index)):
                sent(terms_view(index, cols), r.term_send.at[index, slot])


def per_device(
    x_proj,
    z_proj,
    b_proj,
    c_proj,
    dt_raw,
    dt_bias,
    a_log,
    d_skip,
    conv_x,
    conv_bias_x,
    conv_bc,
    conv_bias_bc,
    norm_weight,
    out_weight,
):
    count = lax.axis_size("seq")
    heads = lax.axis_size("head")
    outer = count // INNER
    rows = x_proj.shape[0]
    tokens = rows * heads
    cols = x_proj.shape[1] // heads
    groups = b_proj.shape[1] // heads // STATE
    width = cols // groups
    local_heads = dt_bias.shape[0]
    blocks = tokens // SPAN
    part = width // INNER
    depth, tile = out_weight.shape
    passes = max(relay_passes(outer), 1)
    dtype = x_proj.dtype
    f32 = jnp.float32
    vmem = pl.BlockSpec(memory_space=pltpu.VMEM)
    smem = pl.BlockSpec(memory_space=pltpu.SMEM)
    hbm = pl.BlockSpec(memory_space=pl.ANY)
    dma = pltpu.SemaphoreType.DMA
    inputs = {
        "x_in": (x_proj, hbm),
        "z_in": (z_proj, hbm),
        "b_in": (b_proj, hbm),
        "c_in": (c_proj, hbm),
        "dt_in": (dt_raw, hbm),
        "w_in": (out_weight, hbm),
        "dt_bias": (dt_bias[None], vmem),
        "a_log": (a_log[None], vmem),
        "skip": (d_skip, smem),
        "conv_x": (conv_x, vmem),
        "bias_x": (conv_bias_x[None], vmem),
        "conv_bc": (conv_bc, vmem),
        "bias_bc": (conv_bias_bc, vmem),
        "gain": (norm_weight[None], vmem),
    }
    scratch = {
        "x_buf": pltpu.VMEM((groups, tokens, width), dtype),
        "z_buf": pltpu.VMEM((groups, tokens, width), dtype),
        "b_buf": pltpu.VMEM((groups, tokens, STATE), dtype),
        "c_buf": pltpu.VMEM((groups, tokens, STATE), dtype),
        "dt_buf": pltpu.VMEM((tokens, dt_raw.shape[1]), dtype),
        "x_halo": pltpu.VMEM((HALO, cols), dtype),
        "b_halo": pltpu.VMEM((HALO, groups * STATE), dtype),
        "c_halo": pltpu.VMEM((HALO, groups * STATE), dtype),
        "wv": pltpu.VMEM((outer, depth, tile), dtype),
        "params": pltpu.VMEM((LANES, LANES), f32),
        "dt_t": pltpu.VMEM((dt_raw.shape[1], SPAN), f32),
        "step_t": pltpu.VMEM((local_heads, tokens), f32),
        "cum_t": pltpu.VMEM((local_heads, tokens), f32),
        "cum_pad": pltpu.VMEM((LANES, SPAN), f32),
        "cum_c": pltpu.VMEM((groups, tokens, LANES), f32),
        "log_out": pltpu.VMEM((8, LANES), f32),
        "log_in": pltpu.VMEM((INNER, 8, LANES), f32),
        "x_pad": pltpu.VMEM((tokens + 8, width), f32),
        "bc_pad": pltpu.VMEM((tokens + 8, STATE), f32),
        "x_t": pltpu.VMEM((width, SPAN), f32),
        "x_w": pltpu.VMEM((width, SPAN), dtype),
        "c_conv": pltpu.VMEM((groups, tokens, STATE), dtype),
        "y_t": pltpu.VMEM((groups, blocks, width, SPAN), f32),
        "pieces": pltpu.VMEM((groups, max(blocks - 1, 1), width, STATE), f32),
        "final": pltpu.VMEM((width, STATE), f32),
        "running": pltpu.VMEM((width, STATE), f32),
        "final_out": pltpu.VMEM((groups, width, STATE), dtype),
        "piece_in": pltpu.VMEM((groups, INNER, part, STATE), dtype),
        "chain_in": pltpu.VMEM((groups, part, STATE), dtype),
        "chain_out": pltpu.VMEM((groups, part, STATE), dtype),
        "start_out": pltpu.VMEM((groups, INNER, part, STATE), dtype),
        "start_in": pltpu.VMEM((groups, width, STATE), dtype),
        "a_buf": pltpu.VMEM((groups, INNER * tokens, width), dtype),
        "acc": pltpu.VMEM((INNER * tokens, tile), f32),
        "terms": pltpu.VMEM((outer, INNER * tokens, tile), dtype),
        "landed": pltpu.VMEM((heads, count, rows, tile), dtype),
        "entry_send": dma((4, max(heads - 1, 1))),
        "entry_recv": dma((4, max(heads - 1, 1), groups)),
        "own_sems": dma((4, groups)),
        "stage": pltpu.VMEM((rows, count * tile), dtype),
        "misc_sems": dma((3,)),
        "spare": dma((1,)),
        "dt_send": dma((heads,)),
        "dt_recv": dma((heads,)),
        "halo_send": dma((3, heads)),
        "halo_recv": dma((3,)),
        "weight_send": dma((2, passes)),
        "weight_recv": dma((outer, CHUNKS)),
        "log_sems": dma((2,)),
        "piece_send": dma((1,)),
        "piece_recv": dma((groups,)),
        "chain_send": dma((1,)),
        "chain_recv": dma((groups,)),
        "start_send": dma((1,)),
        "start_recv": dma((groups,)),
        "share_send": dma((1,)),
        "share_recv": dma((groups,)),
        "near_recv": dma((2,)),
        "term_send": dma((outer, column_halves(tile))),
        "term_recv": dma((outer, column_halves(tile))),
    }
    names = list(inputs) + ["out"] + list(scratch)
    return pl.pallas_call(
        functools.partial(mixer_kernel, count, heads, names),
        out_shape=jax.ShapeDtypeStruct((rows, count * tile), dtype),
        in_specs=[spec for _, spec in inputs.values()],
        out_specs=hbm,
        scratch_shapes=list(scratch.values()),
        compiler_params=pltpu.CompilerParams(
            collective_id=0, has_side_effects=True, vmem_limit_bytes=60 * 1024 * 1024
        ),
        name="mixer",
    )(*[value for value, _ in inputs.values()])


def solution(mesh):
    in_specs = (
        P(("seq", "head"), None),
        P(("seq", "head"), None),
        P(("seq", "head"), None),
        P(("seq", "head"), None),
        P(("seq", "head"), None),
        P("head"),
        P("head"),
        P("head"),
        P(None, "head"),
        P("head"),
        P(None, None, "head"),
        P(None, "head"),
        P("head"),
        P("head", "seq"),
    )
    out_specs = P(("seq", "head"), None)
    return jax.shard_map(
        per_device, mesh=mesh, in_specs=in_specs, out_specs=out_specs, check_vma=False
    )
```
